128 devices in a mesh: row: 8 (over y, core), col: 4 (over z), mp: 4 (over x).
Axes of the slice: x: 4, y: 4, z: 4, core: 2. Of those that a mesh axis runs over, the one named last changes fastest.
Arguments:
- hidden: bfloat16 [32768, 3584], P(('row', 'col'), 'mp'), may hold values from -6 to 6
- old_logp: float32 [32768], P(('row', 'col')), may hold values from -0.6 to 0.6
- rewards: float32 [256], P(('row', 'col')), may hold values from -4 to 4
- resp_dest: int32 [256], P(('row', 'col')), may hold values from 0 to 31, as said below
- resp_len: int32 [256], P(('row', 'col')), may hold values from 1 to 128, as said below
- resp_offset: int32 [256], P(('row', 'col')), may hold values from 0 to 511, as said below
- prompt_group: int32 [256], P(('row', 'col')), may hold values from 0 to 31, as said below
- attn_gain: bfloat16 [3584], replicated, may hold values from 0.099609375 to 1.8984375
- w_query: bfloat16 [3584, 3584], P(None, 'mp'), may hold values from -0.09375 to 0.09375
- q_bias: bfloat16 [3584], P('mp'), may hold values from -3 to 3
- w_key: bfloat16 [3584, 512], P(None, 'mp'), may hold values from -0.09375 to 0.09375
- k_bias: bfloat16 [512], P('mp'), may hold values from -6 to 6
- w_value: bfloat16 [3584, 512], P(None, 'mp'), may hold values from -0.09375 to 0.09375
- v_bias: bfloat16 [512], P('mp'), may hold values from -3 to 3
- w_out: bfloat16 [3584, 3584], P('mp'), may hold values from -0.5 to 0.5
- final_gain: bfloat16 [3584], replicated, may hold values from 0.099609375 to 1.8984375
- chosen_rows: bfloat16 [16384, 3584], P(('row', 'col', 'mp')), may hold values from -0.01171875 to 0.01171875
- log_normalizer: float32 [16384], P(('row', 'col', 'mp')), may hold values from -0.6 to 0.6
Outputs:
- objective: float32 [16384], P(('row', 'col', 'mp'))
- loss: float32 [], replicated
The draws below stay inside these ranges and needn't reach their ends.
Inputs may be any that keep to these rules, and one draw needn't show every extreme that they name: `resp_dest`: ranks are numbered row index * 4 + col index. A rank's responses go to ranks of the same col index: exactly 1 of them to each such rank, itself included; so every rank receives exactly 8 responses. `resp_len`: the responses bound for one rank hold at most 512 tokens together; in every draw some rank's responses fill all 512 positions, and some response has exactly 128. `resp_offset`: responses bound for one rank lie end to end from position 0, without gaps or intersection. `prompt_group`: each of the 32 groups has exactly 8 responses.
All inputs are finite; a program needn't handle non-finite values.
Results may differ from the reference program's by a relative error of at most 0.0019.
Values may be sent and summed in bfloat16 or wider, within the bound.
No kernel may reach another device: no remote copies, remote signals or barrier semaphores. Data moves between devices by JAX's collectives and lax.ppermute only.
A program may use at most 128 MiB of HBM per device.

```python
import jax
import jax.numpy as jnp
from jax import lax

D = 3584
HEADS = 28
KV_HEADS = 4
HEAD = 128
MAXLEN = 128
RESP_DEV = 8
GROUP_SIZE = 8
RANKS = 32
RESPONSES = 256
PACK = 512
N_ROW = 8
N_COL = 4
N_MP = 4


def routing_plan(key):
    base_key = jax.random.fold_in(key, 4242)
    key_list = jax.random.split(base_key, 7)
    per_peer = RESP_DEV // N_ROW
    source_keys = jax.random.split(key_list[0], RANKS)
    shuffles = jax.vmap(lambda one_key: jax.random.permutation(one_key, RESP_DEV))(source_keys)
    source_ids = jnp.arange(RANKS, dtype=jnp.int32)[:, None]
    source_row = source_ids // N_COL
    source_col = source_ids % N_COL
    dest_row = shuffles // per_peer
    slot_in_peer = shuffles % per_peer
    targets = dest_row * N_COL + source_col
    arrival = source_row * per_peer + slot_in_peer
    levels = jax.random.randint(key_list[3], (RANKS, RESP_DEV), 0, 5)
    base_length = jnp.right_shift(jnp.full((RANKS, RESP_DEV), MAXLEN, jnp.int32), levels)
    jitter = jax.random.randint(key_list[4], (RANKS, RESP_DEV), 0, 1 << 20) % (base_length // 4 + 1)
    drawn = jnp.maximum(base_length - jitter, 1)
    chosen_rank = jax.random.randint(key_list[5], (), 0, RANKS)
    chosen_slot = jax.random.randint(key_list[6], (), 0, RESP_DEV - 1)
    extra_slot = (chosen_slot + 1) % (RESP_DEV - 1)
    slot_ids = jnp.arange(RESP_DEV, dtype=jnp.int32)[None, :]
    rank_hit = jnp.arange(RANKS, dtype=jnp.int32)[:, None] == chosen_rank
    rest_tokens = PACK - 1 - MAXLEN
    filler_count = RESP_DEV - 2
    filler = rest_tokens // filler_count
    leftover = rest_tokens % filler_count
    full_row = jnp.where(slot_ids == RESP_DEV - 1, 1, jnp.where(slot_ids == chosen_slot, MAXLEN, filler + jnp.where(slot_ids == extra_slot, leftover, 0)))
    drawn = jnp.where(rank_hit, full_row, drawn).astype(jnp.int32)
    totals = jnp.sum(drawn, 1, keepdims=True)
    lengths = jnp.where(totals > PACK, jnp.maximum(drawn // 2, 1), drawn)
    offsets = jnp.cumsum(lengths, 1) - lengths
    return (targets.reshape(-1).astype(jnp.int32), lengths[targets, arrival].reshape(-1).astype(jnp.int32), offsets[targets, arrival].reshape(-1).astype(jnp.int32))


def draw_resp_dest(key, part):
    return routing_plan(key)[0]


def draw_resp_len(key, part):
    return routing_plan(key)[1]


def draw_resp_offset(key, part):
    return routing_plan(key)[2]


def draw_prompt_group(key, part):
    shuffled = jax.random.permutation(jax.random.fold_in(key, 77), RANKS * RESP_DEV)
    return (shuffled // GROUP_SIZE).astype(jnp.int32)


def steps_of(rng, dims, cuts, smallest, largest):
    def one(axis_at, shards_of):
        draws = jax.random.uniform(jax.random.fold_in(jax.random.fold_in(rng, 6), axis_at), (shards_of,), jnp.float32, smallest / len(cuts), largest / len(cuts))
        return jnp.repeat(jnp.exp(draws), dims[axis_at] // shards_of).reshape((-1,) + (1,) * (len(dims) - axis_at - 1))

    level = one(*cuts[0])
    for cut in cuts[1:]:
        level = level * one(*cut)
    return level


def gaussian(stream_key, shape, scale, limit, shards=(), kind=jnp.bfloat16):
    result = jax.random.normal(stream_key, shape, jnp.float32) * scale
    if len(shards) > 0:
        result = steps_of(stream_key, shape, shards, -0.22, 0.18) * result
    return jnp.clip(result, min=-limit, max=limit).astype(kind)


def setup_inputs(seed: int = 0) -> dict:
    key_of = jax.random.split(jax.random.key(seed), 19)
    return {
        "hidden": gaussian(key_of[0], (RESPONSES * MAXLEN, D), 1.0, 6.0, ((0, 32), (1, 4))),
        "old_logp": gaussian(key_of[1], (RESPONSES * MAXLEN,), 0.1, 0.6, ((0, 32),), jnp.float32),
        "rewards": gaussian(key_of[2], (RESPONSES,), 1.0, 4.0, ((0, 32),), jnp.float32),
        "resp_dest": draw_resp_dest(jax.random.fold_in(key_of[18], 71), 0),
        "resp_len": draw_resp_len(jax.random.fold_in(key_of[18], 71), 0),
        "resp_offset": draw_resp_offset(jax.random.fold_in(key_of[18], 71), 0),
        "prompt_group": draw_prompt_group(jax.random.fold_in(key_of[18], 71), 0),
        "attn_gain": jnp.clip(1.0 + 0.18 * jax.random.normal(key_of[7], (D,), jnp.float32), 0.099609375, 1.8984375).astype(jnp.bfloat16),
        "w_query": gaussian(key_of[8], (D, HEADS * HEAD), D ** -0.5, 0.09375, ((1, 4),)),
        "q_bias": gaussian(key_of[9], (HEADS * HEAD,), 0.5, 3.0, ((0, 4),)),
        "w_key": gaussian(key_of[10], (D, KV_HEADS * HEAD), D ** -0.5, 0.09375, ((1, 4),)),
        "k_bias": gaussian(key_of[11], (KV_HEADS * HEAD,), 1.0, 6.0, ((0, 4),)),
        "w_value": gaussian(key_of[12], (D, KV_HEADS * HEAD), D ** -0.5, 0.09375, ((1, 4),)),
        "v_bias": gaussian(key_of[13], (KV_HEADS * HEAD,), 0.5, 3.0, ((0, 4),)),
        "w_out": gaussian(key_of[14], (HEADS * HEAD, D), HEAD ** -0.5, 0.5, ((0, 4),)),
        "final_gain": jnp.clip(1.0 + 0.18 * jax.random.normal(key_of[15], (D,), jnp.float32), 0.099609375, 1.8984375).astype(jnp.bfloat16),
        "chosen_rows": gaussian(key_of[16], (RANKS * PACK, D), (64 * D) ** -0.5, 0.01171875, ((0, 128),)),
        "log_normalizer": gaussian(key_of[17], (RANKS * PACK,), 0.1, 0.6, ((0, 128),), jnp.float32),
    }


norm_eps = 1e-06
rope_theta = 1000000.0
clip_low = 0.2
clip_high = 0.28
std_floor = 1.0
mask_fill = -1e+30

def rotary(matrix, positions):
    half_size = matrix.shape[-1] // 2
    exponents = jnp.arange(half_size, dtype=jnp.float32) * (2.0 / matrix.shape[-1])
    frequency = rope_theta ** (-exponents)
    angles = positions[:, None] * frequency[None, :]
    cosine_table = jnp.cos(angles)[:, None, :]
    sine_table = jnp.sin(angles)[:, None, :]
    first_half = matrix[..., :half_size]
    second_half = matrix[..., half_size:]
    return jnp.concatenate([first_half * cosine_table - second_half * sine_table, second_half * cosine_table + first_half * sine_table], -1)

def reference(hidden, old_logp, rewards, resp_dest, resp_len, resp_offset, prompt_group, attn_gain, w_query, q_bias, w_key, k_bias, w_value, v_bias, w_out, final_gain, chosen_rows, log_normalizer):
    highest = lax.Precision.HIGHEST
    group_total = RESPONSES // GROUP_SIZE
    member = (prompt_group[:, None] == jnp.arange(group_total, dtype=jnp.int32)[None, :]).astype(jnp.float32)
    group_mean = jnp.dot(rewards, member, precision=highest) / GROUP_SIZE
    centered = rewards - jnp.dot(member, group_mean, precision=highest)
    spread = jnp.dot(centered * centered, member, precision=highest) / GROUP_SIZE
    group_scale = jnp.maximum(jnp.sqrt(spread), std_floor)
    advantage = centered / jnp.dot(member, group_scale, precision=highest)
    response_ids = jnp.arange(RESPONSES, dtype=jnp.int32)[None, :]
    slots = jnp.arange(PACK, dtype=jnp.int32)[:, None]

    def one_rank(dest_rank):
        covered = (resp_dest[None, :] == dest_rank) & (slots >= resp_offset[None, :]) & (slots < resp_offset[None, :] + resp_len[None, :])
        occupied = jnp.any(covered, 1)
        within_all = slots - resp_offset[None, :]
        token_index = lax.optimization_barrier(jnp.sum(jnp.where(covered, response_ids * MAXLEN + within_all, 0), 1)).astype(jnp.int32)
        positions = lax.optimization_barrier(jnp.sum(jnp.where(covered, within_all, 0), 1)).astype(jnp.float32)
        segment = jnp.where(occupied, lax.optimization_barrier(jnp.sum(jnp.where(covered, response_ids, 0), 1)), -1)
        token_adv = lax.optimization_barrier(jnp.sum(jnp.where(covered, advantage[None, :], 0.0), 1))
        packed = jnp.where(occupied[:, None], hidden[token_index], jnp.zeros((), hidden.dtype))
        wide = packed.astype(jnp.float32)
        inverse = lax.rsqrt(lax.optimization_barrier(jnp.mean(wide * wide, -1, keepdims=True)) + norm_eps)
        normed = (wide * inverse * attn_gain.astype(jnp.float32)).astype(jnp.bfloat16)
        queries = jnp.dot(normed, w_query, preferred_element_type=jnp.float32) + q_bias.astype(jnp.float32)
        queries = rotary(queries.reshape(PACK, HEADS, HEAD), positions).astype(jnp.bfloat16)
        key_rows = jnp.dot(normed, w_key, preferred_element_type=jnp.float32) + k_bias.astype(jnp.float32)
        key_rows = rotary(key_rows.reshape(PACK, KV_HEADS, HEAD), positions).astype(jnp.bfloat16)
        value_rows = (jnp.dot(normed, w_value, preferred_element_type=jnp.float32) + v_bias.astype(jnp.float32)).astype(jnp.bfloat16).reshape(PACK, KV_HEADS, HEAD)
        grouped = queries.reshape(PACK, KV_HEADS, HEADS // KV_HEADS, HEAD).astype(jnp.float32)
        scores = jnp.einsum('qkgd,ekd->kgqe', grouped, key_rows.astype(jnp.float32)) * HEAD ** (-0.5)
        order_ids = jnp.arange(PACK, dtype=jnp.int32)
        allowed = (segment[:, None] == segment[None, :]) & (order_ids[None, :] <= order_ids[:, None])
        scores = jnp.where(allowed, scores, mask_fill)
        highest_score = lax.optimization_barrier(jnp.max(scores, -1, keepdims=True))
        exponent = jnp.exp(scores - highest_score)
        weights = (exponent / lax.optimization_barrier(jnp.sum(exponent, -1, keepdims=True))).astype(jnp.bfloat16)
        mixed = jnp.einsum('kgqe,ekd->qkgd', weights.astype(jnp.float32), value_rows.astype(jnp.float32))
        mixed = mixed.reshape(PACK, HEADS * HEAD).astype(jnp.bfloat16)
        partial_value = jnp.einsum('pgx,gxd->gpd', mixed.reshape(PACK, N_MP, -1).astype(jnp.float32), w_out.reshape(N_MP, -1, D).astype(jnp.float32)).astype(jnp.bfloat16)
        branch = lax.optimization_barrier(jnp.sum(partial_value.astype(jnp.float32), 0))
        residual_out = (wide + branch).astype(jnp.bfloat16)
        final_rows = residual_out.astype(jnp.float32)
        final_inverse = lax.rsqrt(lax.optimization_barrier(jnp.mean(final_rows * final_rows, -1, keepdims=True)) + norm_eps)
        first_row = (dest_rank * PACK).astype(jnp.int32)
        chosen = lax.dynamic_slice_in_dim(chosen_rows, first_row, PACK, 0).astype(jnp.float32)
        normalizer = lax.dynamic_slice_in_dim(log_normalizer, first_row, PACK, 0)
        logits = lax.optimization_barrier(jnp.sum(final_rows * final_inverse * final_gain.astype(jnp.float32) * chosen, -1))
        old_values = jnp.where(occupied, old_logp[token_index], 0.0)
        ratios = jnp.exp(logits - normalizer - old_values)
        bounded = jnp.clip(ratios, 1.0 - clip_low, 1.0 + clip_high)
        objective = jnp.where(occupied, jnp.minimum(ratios * token_adv, bounded * token_adv), 0.0)
        return (objective, occupied.astype(jnp.float32))
    objective, counted = lax.map(one_rank, jnp.arange(RANKS, dtype=jnp.int32))
    objective = objective.reshape(-1)
    loss = -jnp.sum(objective) / jnp.sum(counted)
    return (objective, loss)
```

```python
import functools

import jax
import jax.numpy as jnp
from jax import lax
from jax.experimental import pallas as pl
from jax.experimental.pallas import tpu as pltpu
from jax.sharding import PartitionSpec as P


HEAD = 128
GROUP_SIZE = 8
SLOT = 128
ROWS = 8
COLS = 4
SHARDS = 4
PACK = 512
ROW_COL = ("row", "col")
ROW_COL_MP = ("row", "col", "mp")
CHUNKS = (384, 512)
STARTS = (0, 384)

norm_eps = 1e-06
rope_theta = 1000000.0
clip_low = 0.2
clip_high = 0.28
std_floor = 1.0
mask_fill = -1e30

F32 = jnp.float32
BF16 = jnp.bfloat16
VMEM = pl.BlockSpec(memory_space=pltpu.VMEM)
SMEM = pl.BlockSpec(memory_space=pltpu.SMEM)
HBM = pl.BlockSpec(memory_space=pltpu.HBM)


def call(kernel, out_shape, in_specs, args, *, flops, size, scratch=(), limit=16 << 20):
    return pl.pallas_call(
        kernel,
        out_shape=out_shape,
        in_specs=in_specs,
        out_specs=jax.tree.map(lambda _: VMEM, out_shape),
        scratch_shapes=list(scratch),
        compiler_params=pltpu.CompilerParams(vmem_limit_bytes=limit),
        cost_estimate=pl.CostEstimate(flops=flops, bytes_accessed=size, transcendentals=0),
    )(*args)


def shape(*dims, dtype=BF16):
    return jax.ShapeDtypeStruct(dims, dtype)


def in_hbm(value):
    return pltpu.with_memory_space_constraint(value, pltpu.HBM)


def in_vmem(value):
    return pltpu.with_memory_space_constraint(value, pltpu.VMEM)


def shift(value, axis, size, by):
    return lax.ppermute(value, axis, [(i, (i + by) % size) for i in range(size)])


def three_parts(value):
    high = value.astype(BF16).astype(F32)
    middle = (value - high).astype(BF16).astype(F32)
    return high, middle, value - high - middle


def by_row(rows):
    sub = lax.broadcasted_iota(jnp.int32, (8, SLOT), 0)
    tile = jnp.zeros((8, SLOT), F32)
    for n, value in enumerate(rows):
        tile = jnp.where(sub == n, value, tile)
    return tile


def send_kernel(*refs):
    sources, hidden, outs = refs[:6], refs[6], refs[7:-9]
    *held, order, small, sems = refs[-9:]
    row = lax.axis_index("row").astype(jnp.int32)
    loads = [pltpu.make_async_copy(a, b, small.at[i]) for i, (a, b) in enumerate(zip(sources, held))]
    for load in loads:
        load.start()
    for load in loads:
        load.wait()
    dest_of, length_of, offset_of, group_of, reward_of, old_logp = held
    for slot in range(ROWS):
        order[lax.rem(lax.shift_right_logical(dest_of[slot], 2) - row + ROWS, ROWS)] = slot
    copies = []
    for c in range(len(CHUNKS)):
        for k in range(ROWS):
            copies.append(
                pltpu.make_async_copy(
                    hidden.at[
                        pl.ds(pl.multiple_of(order[k] * SLOT, SLOT), SLOT),
                        pl.ds(STARTS[c], CHUNKS[c]),
                    ],
                    outs[c * ROWS + k].at[pl.ds(0, SLOT), :],
                    sems.at[c * ROWS + k],
                )
            )
            copies[-1].start()
    lane = lax.broadcasted_iota(jnp.int32, (1, SLOT), 1)
    shared = []
    for entries in (reward_of, group_of, length_of):
        value = jnp.zeros((1, SLOT), F32)
        for i in range(ROWS):
            value = jnp.where(lane == i, entries[i].astype(F32), value)
        shared.append(value)
    for k in range(ROWS):
        slot = order[k]
        place = offset_of[slot]
        high = lax.shift_right_logical(place, 4)
        low = place - high * 16
        own = by_row(
            (
                length_of[slot].astype(F32),
                high.astype(F32),
                low.astype(F32),
                *three_parts(old_logp[pl.ds(slot, 1), :]),
            )
        )
        common = by_row((*three_parts(shared[0]), shared[1], shared[2], slot.astype(F32)))
        outs[k][SLOT : SLOT + 8, 0:SLOT] = own.astype(BF16)
        outs[k][SLOT : SLOT + 8, SLOT : 2 * SLOT] = common.astype(BF16)
        if CHUNKS[0] > 2 * SLOT:
            outs[k][SLOT : SLOT + 8, 2 * SLOT :] = jnp.zeros((8, CHUNKS[0] - 2 * SLOT), BF16)
    for copy in copies:
        copy.wait()


def send_blocks(*args):
    outs = [shape(SLOT + (8 if c == 0 else 0), CHUNKS[c]) for c in range(len(CHUNKS)) for _ in range(ROWS)]
    flat = call(
        send_kernel,
        outs,
        [HBM] * 7,
        [in_hbm(a) for a in args],
        flops=1000000,
        size=4 << 20,
        scratch=[
            *[pltpu.SMEM((ROWS,), jnp.int32)] * 4,
            pltpu.SMEM((ROWS,), F32),
            pltpu.VMEM((ROWS, SLOT), F32),
            pltpu.SMEM((ROWS,), jnp.int32),
            pltpu.SemaphoreType.DMA((6,)),
            pltpu.SemaphoreType.DMA((len(outs),)),
        ],
    )
    return [flat[c * ROWS : (c + 1) * ROWS] for c in range(len(CHUNKS))]


def fetch_kernel(*refs):
    count = (len(refs) - 1) // 2
    copies = [pltpu.make_async_copy(refs[i], refs[count + i], refs[-1].at[i]) for i in range(count)]
    for copy in copies:
        copy.start()
    for copy in copies:
        copy.wait()


def fetch(*values):
    return call(
        fetch_kernel,
        [pltpu.VMEM(v.shape, v.dtype) for v in values],
        [HBM] * len(values),
        [in_hbm(v) for v in values],
        flops=1000,
        size=8 << 20,
        scratch=[pltpu.SemaphoreType.DMA((len(values),))],
    )


def pack_kernel(first, *refs):
    blocks = refs[:ROWS]
    if first:
        upper, lower, positions, notes = refs[ROWS:]
    else:
        notes, upper, lower = refs[ROWS:]
    place = lax.broadcasted_iota(jnp.int32, (PACK, SLOT), 0).astype(F32)
    lane = lax.broadcasted_iota(jnp.int32, (PACK, SLOT), 1).astype(F32)
    picks = []
    within = jnp.zeros((PACK, SLOT), F32)
    for k in range(ROWS):
        if first:
            notes[8 * k : 8 * k + 8, :] = blocks[k][SLOT : SLOT + 8, 0 : 2 * SLOT]
            note = blocks[k][SLOT : SLOT + 8, 0:SLOT].astype(F32)
        else:
            note = notes[8 * k : 8 * k + 8, 0:SLOT].astype(F32)
        length = note[0:1, :]
        offset = note[1:2, :] * 16.0 + note[2:3, :]
        hit = (place - offset == lane) & (lane < length)
        picks.append(jnp.where(hit, 1.0, 0.0).astype(BF16))
        if first:
            within = within + jnp.where(hit, lane, 0.0)
    pick = jnp.concatenate(picks, 1)
    rows = jnp.concatenate([b[0:SLOT, :] for b in blocks], 0)
    packed = jnp.dot(pick, rows, preferred_element_type=F32).astype(BF16)
    upper[...] = packed[: PACK // 2]
    lower[...] = packed[PACK // 2 :]
    if first:
        positions[...] = jnp.broadcast_to(jnp.sum(within, 1, keepdims=True), (PACK, SLOT))


def pack(c, blocks, notes=None):
    outs = [shape(PACK // 2, CHUNKS[c]), shape(PACK // 2, CHUNKS[c])]
    args = list(blocks)
    if notes is None:
        outs += [shape(PACK, SLOT, dtype=F32), shape(8 * ROWS, 2 * SLOT)]
    else:
        args.append(notes)
    return call(
        functools.partial(pack_kernel, notes is None),
        outs,
        [VMEM] * len(args),
        args,
        flops=2 * PACK * 8 * SLOT * CHUNKS[c],
        size=2 << 20,
    )


def gather_halves(upper, lower):
    left_upper = shift(upper, "mp", SHARDS, 1)
    right_lower = shift(lower, "mp", SHARDS, -1)
    left_lower = shift(lower, "mp", SHARDS, 1)
    right_upper = shift(upper, "mp", SHARDS, -1)
    far_upper = shift(left_upper, "mp", SHARDS, 1)
    far_lower = shift(right_lower, "mp", SHARDS, -1)
    return {
        0: (upper, lower),
        3: (left_upper, left_lower),
        1: (right_upper, right_lower),
        2: (far_upper, far_lower),
    }


def project_kernel(c, steps, carried, last, *refs):
    width = CHUNKS[c]
    refs = list(refs)
    halves = [(refs.pop(0), refs.pop(0)) for _ in steps]
    gain, w_query, w_key, w_value = [refs.pop(0) for _ in range(4)]
    if carried:
        total_in, square_in = refs.pop(0), refs.pop(0)
    if last:
        bias, cosine, sine = refs.pop(0), refs.pop(0), refs.pop(0)
        queries, keys, values = refs.pop(0), refs.pop(0), refs.pop(0)
    else:
        total_out, square_out = refs.pop(0), refs.pop(0)
    own = refs
    me = lax.axis_index("mp").astype(jnp.int32)
    begin = pl.multiple_of(lax.rem(me, 2) * SLOT, SLOT)
    for i, (upper, lower) in enumerate(halves):
        own[i][...] = jnp.where(
            me < 2, upper[pl.ds(begin, SLOT), :], lower[pl.ds(begin, SLOT), :]
        )
    half = PACK // 2
    sources = [lax.rem(me + step, SHARDS) for step in steps]
    features = gain.shape[1]
    picked = [
        pl.ds(pl.multiple_of(source * features + STARTS[c], SLOT), width) for source in sources
    ]

    def weights(i, tile):
        if tile < 3:
            return w_query[picked[i], tile * 256 : tile * 256 + 256]
        if tile == 3:
            return jnp.concatenate([w_query[picked[i], 768:896], w_key[picked[i], :]], 1)
        return w_value[picked[i], :]

    for h in range(2):
        rows = slice(h * half, (h + 1) * half)
        square = jnp.zeros((half, SLOT), F32)
        scaled = []
        for i, pair in enumerate(halves):
            wide = pair[h][...].astype(F32)
            for j in range(0, width, SLOT):
                square = square + wide[:, j : j + SLOT] * wide[:, j : j + SLOT]
            factor = gain[pl.ds(sources[i], 1), STARTS[c] : STARTS[c] + width]
            scaled.append((wide * factor).astype(BF16))
        if carried:
            square = square + square_in[rows, :]
        if last:
            mean = jnp.sum(square, 1, keepdims=True) * (1.0 / (SHARDS * features))
            inverse = lax.rsqrt(mean + norm_eps)
        else:
            square_out[rows, :] = square
        for tile in range(5):
            columns = slice(tile * 256, min(tile * 256 + 256, 9 * HEAD))
            part = None
            for i in range(len(steps)):
                term = jnp.dot(scaled[i], weights(i, tile), preferred_element_type=F32)
                part = term if part is None else part + term
            if carried:
                part = part + total_in[rows, columns]
            if not last:
                total_out[rows, columns] = part
                continue
            part = part * inverse + bias[0:1, columns]
            for n in range(part.shape[1] // HEAD):
                head = part[:, n * HEAD : (n + 1) * HEAD]
                at = 2 * tile + n
                if at < 8:
                    head = head * cosine[rows, :] + pltpu.roll(head, HEAD // 2, 1) * sine[rows, :]
                if at < 7:
                    queries[rows, at * HEAD : (at + 1) * HEAD] = head.astype(BF16)
                elif at == 7:
                    keys[rows, :] = head.astype(BF16)
                else:
                    values[rows, :] = head.astype(BF16)


def project(c, steps, pieces, weights, carried=None, tables=None):
    width = CHUNKS[c]
    columns = 9 * HEAD
    args = []
    for step in steps:
        args += list(pieces[step])
    args += list(weights)
    if carried is not None:
        args += list(carried)
    if tables is None:
        outs = [shape(PACK, columns, dtype=F32), shape(PACK, SLOT, dtype=F32)]
    else:
        args += list(tables)
        outs = [shape(PACK, 7 * HEAD), shape(PACK, HEAD), shape(PACK, HEAD)]
    keep = len(outs)
    outs += [shape(SLOT, width)] * len(steps)
    result = call(
        functools.partial(project_kernel, c, steps, carried is not None, tables is not None),
        outs,
        [VMEM] * len(args),
        args,
        flops=2 * PACK * width * len(steps) * columns,
        size=len(steps) * width * (columns + PACK) * 2 + (4 << 20),
    )
    return result[:keep], dict(zip(steps, result[keep:]))


def attend_kernel(steps, queries, keys, values, positions, w_out, *outs):
    me = lax.axis_index("mp").astype(jnp.int32)
    heads = queries.shape[1] // HEAD
    for n, step in enumerate(steps):
        block = lax.rem(me + step, SHARDS)
        begin = pl.multiple_of(block * SLOT, SLOT)
        window = pl.multiple_of(jnp.maximum(block - 1, 0) * SLOT, SLOT)
        row = begin.astype(F32) + lax.broadcasted_iota(jnp.int32, (SLOT, SLOT), 0).astype(F32)
        lane = window.astype(F32) + lax.broadcasted_iota(jnp.int32, (SLOT, SLOT), 1).astype(F32)
        row_start = row - positions[pl.ds(begin, SLOT), :]
        allowed = jnp.concatenate(
            [(lane >= row_start) & (lane <= row), (lane + SLOT >= row_start) & (lane + SLOT <= row)], 1
        )
        all_keys = keys[pl.ds(window, 2 * SLOT), :]
        all_values = values[pl.ds(window, 2 * SLOT), :]
        mixed = []
        for h in range(heads):
            scores = lax.dot_general(
                queries[pl.ds(begin, SLOT), h * HEAD : (h + 1) * HEAD],
                all_keys,
                (((1,), (1,)), ((), ())),
                preferred_element_type=F32,
            )
            scores = jnp.where(allowed, scores * HEAD ** (-0.5), mask_fill)
            exponent = jnp.exp(scores - jnp.max(scores, 1, keepdims=True))
            weights = (exponent / jnp.sum(exponent, 1, keepdims=True)).astype(BF16)
            mixed.append(
                jnp.dot(weights, all_values, preferred_element_type=F32).astype(BF16)
            )
        mixed = jnp.concatenate(mixed, 1)
        for j in range(0, w_out.shape[1], 512):
            part = jnp.dot(mixed, w_out[:, j : j + 512], preferred_element_type=F32).astype(BF16)
            outs[2 * n][:, j : j + 512] = part[: SLOT // 2]
            outs[2 * n + 1][:, j : j + 512] = part[SLOT // 2 :]


def attend(steps, queries, keys, values, positions, w_out):
    width = w_out.shape[1]
    return call(
        functools.partial(attend_kernel, steps),
        [shape(SLOT // 2, width)] * (2 * len(steps)),
        [VMEM] * 5,
        (queries, keys, values, positions, w_out),
        flops=len(steps) * 2 * SLOT * w_out.shape[0] * (width + 4 * SLOT),
        size=8 << 20,
    )


def add_kernel(a, b, c, d, ab, cd):
    ab[...] = (a[...].astype(F32) + b[...].astype(F32)).astype(BF16)
    cd[...] = (c[...].astype(F32) + d[...].astype(F32)).astype(BF16)


def sort_kernel(notes, stats_out, mine_out):
    lane = lax.broadcasted_iota(jnp.int32, (1, SLOT), 1)
    for k in range(ROWS):
        own = notes[8 * k : 8 * k + 8, 0:SLOT].astype(F32)
        common = notes[8 * k : 8 * k + 8, SLOT : 2 * SLOT].astype(F32)
        rewards = common[0:1, :] + common[1:2, :] + common[2:3, :]
        groups = common[3:4, :]
        picked = lane.astype(F32) == common[5:6, :]
        stats_out[k : k + 1, :] = (
            rewards + pltpu.roll(groups, 8, 1) + pltpu.roll(common[4:5, :], 16, 1)
        )
        info = jnp.where(lane == 26, own[1:2, :] * 16.0 + own[2:3, :], 0.0)
        info = jnp.where(lane == 27, own[0:1, :], info)
        for n, value in ((24, rewards), (25, groups)):
            info = jnp.where(
                lane == n, jnp.sum(jnp.where(picked, value, 0.0), 1, keepdims=True), info
            )
        mine_out[k : k + 1, 0:SLOT] = own[3:4, :] + own[4:5, :] + own[5:6, :]
        mine_out[k : k + 1, SLOT:] = info


def note_kernel(stats_a, stats_b, stats_c, stats_d, mine_ref, log_normalizer, base_out, adv_out, occupied_out, scale_out):
    me = lax.axis_index("mp").astype(jnp.int32)
    lane32 = lax.broadcasted_iota(jnp.int32, (COLS * ROWS, SLOT), 1)
    rewards = jnp.concatenate([stats_a[...], stats_b[...], stats_c[...], stats_d[...]], 0)
    groups = pltpu.roll(rewards, SLOT - 8, 1)
    lengths = pltpu.roll(rewards, SLOT - 16, 1)
    valid = lane32 < 8
    place = (lax.broadcasted_iota(jnp.int32, (SLOT, SLOT), 0) + me * SLOT).astype(F32)
    lane_int = lax.broadcasted_iota(jnp.int32, (SLOT, SLOT), 1)
    lane = lane_int.astype(F32)
    one_lane = lax.broadcasted_iota(jnp.int32, (1, SLOT), 1)

    def total(value):
        return jnp.sum(jnp.sum(value, 1, keepdims=True), 0, keepdims=True)

    old = jnp.zeros((SLOT, SLOT), F32)
    adv = jnp.zeros((SLOT, SLOT), F32)
    occupied = jnp.zeros((SLOT, SLOT), F32)
    for r in range(ROWS):
        mine = mine_ref[r : r + 1, :]
        info = mine[:, SLOT:]

        def entry(at):
            return jnp.sum(jnp.where(one_lane == at, info, 0.0), 1, keepdims=True)

        reward, group, offset, length = entry(24), entry(25), entry(26), entry(27)
        member = valid & (groups == group)
        mean = total(jnp.where(member, rewards, 0.0)) / GROUP_SIZE
        centered = jnp.where(member, rewards - mean, 0.0)
        spread = total(centered * centered) / GROUP_SIZE
        advantage = (reward - mean) / jnp.maximum(jnp.sqrt(spread), std_floor)
        hit = (place - offset == lane) & (lane < length)
        old = old + jnp.where(hit, mine[:, :SLOT], 0.0)
        adv = adv + jnp.where(hit, advantage, 0.0)
        occupied = occupied + jnp.where(hit, 1.0, 0.0)
    diagonal = lane_int == lax.broadcasted_iota(jnp.int32, (SLOT, SLOT), 0)
    old = old + jnp.where(diagonal, log_normalizer[...], 0.0)
    base_out[...] = jnp.sum(old, 1, keepdims=True)
    adv_out[...] = jnp.sum(adv, 1, keepdims=True)
    occupied_out[...] = jnp.sum(occupied, 1, keepdims=True)
    scale_out[...] = -1.0 / total(jnp.where(valid, lengths, 0.0))


def prepare_kernel(keys, *refs):
    refs = list(refs)
    own = [refs.pop(0) for _ in keys]
    own_a, raw_a, own_b, raw_b, gain, chosen, known, factor = refs
    me = lax.axis_index("mp").astype(jnp.int32)
    for (c, step), resid in zip(keys, own):
        start = lax.rem(me + step, SHARDS) * sum(CHUNKS) + STARTS[c]
        for j in range(0, CHUNKS[c], SLOT):
            at = pl.ds(pl.multiple_of(start + j, SLOT), SLOT)
            branch = jnp.concatenate(
                [
                    own_a[:, at].astype(F32) + raw_a[:, at].astype(F32),
                    own_b[:, at].astype(F32) + raw_b[:, at].astype(F32),
                ],
                0,
            )
            known[:, at] = resid[:, j : j + SLOT].astype(F32) + branch
    factor[...] = gain[...].astype(F32) * chosen[...].astype(F32)


def finish_kernel(known, factor, two_a, two_b, base, adv, occupied, objective_out, total_out):
    width = known.shape[1]
    square = jnp.zeros((SLOT, SLOT), F32)
    product = jnp.zeros((SLOT, SLOT), F32)
    for j in range(0, width, SLOT):
        at = slice(j, j + SLOT)
        two = jnp.concatenate([two_a[:, at].astype(F32), two_b[:, at].astype(F32)], 0)
        rows = (known[:, at] + two).astype(BF16).astype(F32)
        square = square + rows * rows
        product = product + rows * factor[:, at]
    mean = jnp.sum(square, 1, keepdims=True) * (1.0 / width)
    logits = jnp.sum(product, 1, keepdims=True) * lax.rsqrt(mean + norm_eps)
    ratios = jnp.exp(logits - base[...])
    bounded = jnp.clip(ratios, 1.0 - clip_low, 1.0 + clip_high)
    value = jnp.minimum(ratios * adv[...], bounded * adv[...])
    value = jnp.where(occupied[...] > 0.5, value, 0.0)
    diagonal = lax.broadcasted_iota(jnp.int32, (SLOT, SLOT), 1) == lax.broadcasted_iota(
        jnp.int32, (SLOT, SLOT), 0
    )
    line = jnp.sum(jnp.where(diagonal, value, 0.0), 0, keepdims=True)
    objective_out[...] = line
    total = jnp.sum(line, 1, keepdims=True)
    total_out[...] = jnp.broadcast_to(total[None], (SLOT, 1, SLOT))


def body(
    hidden,
    old_logp,
    rewards,
    resp_dest,
    resp_len,
    resp_offset,
    prompt_group,
    attn_gain,
    w_query,
    q_bias,
    w_key,
    k_bias,
    w_value,
    v_bias,
    w_out,
    final_gain,
    chosen_rows,
    log_normalizer,
):
    sent = send_blocks(
        resp_dest,
        resp_len,
        resp_offset,
        prompt_group,
        rewards,
        old_logp.reshape(ROWS, SLOT),
        hidden,
    )
    received = [
        [blocks[0]] + [shift(blocks[k], "row", ROWS, k) for k in range(1, ROWS)] for blocks in sent
    ]
    upper, lower, positions, notes = pack(0, received[0])
    first = gather_halves(upper, lower)
    second = gather_halves(*pack(1, received[1], notes))

    gain = attn_gain.astype(F32).reshape(SHARDS, -1)
    last_gain = final_gain[None, :]
    bias = jnp.concatenate([q_bias, k_bias, v_bias]).astype(F32)[None, :]
    exponents = (jnp.arange(HEAD, dtype=F32) % (HEAD // 2)) * (2.0 / HEAD)
    angles = positions * (rope_theta ** (-exponents))[None, :]
    sign = jnp.where(jnp.arange(HEAD) < HEAD // 2, -1.0, 1.0)
    cosine, sine = jnp.cos(angles), jnp.sin(angles) * sign[None, :]
    gain, last_gain, bias, cosine, sine, w_query, w_key, w_value, w_out = lax.optimization_barrier(
        (gain, last_gain, bias, cosine, sine, w_query, w_key, w_value, w_out)
    )
    tables = (bias, cosine, sine)
    weights = (gain, *[in_vmem(w) for w in fetch(w_query, w_key, w_value)])
    w_out = in_vmem(fetch(w_out)[0])
    stats, mine = call(
        sort_kernel,
        [shape(ROWS, SLOT, dtype=F32), shape(ROWS, 2 * SLOT, dtype=F32)],
        [VMEM],
        (notes,),
        flops=100000,
        size=1 << 17,
    )

    carried, own_first = project(0, (0, 1, 3, 2), first, weights)
    carried, own_near = project(1, (0, 1, 3), second, weights, carried)
    (queries, keys, values), own_far = project(1, (2,), second, weights, carried, tables)

    attend_to = functools.partial(
        attend,
        queries=queries,
        keys=keys,
        values=values,
        positions=positions,
        w_out=w_out,
    )
    far_a, far_b = attend_to((2,))
    from_left = shift(far_a, "mp", SHARDS, 1)
    from_right = shift(far_b, "mp", SHARDS, -1)
    right_a, right_b, left_a, left_b = attend_to((1, 3))
    raw_b = shift(right_b, "mp", SHARDS, 1)
    raw_a = shift(left_a, "mp", SHARDS, -1)
    own_a, own_b = attend_to((0,))
    stats, own_a = lax.optimization_barrier((stats, own_a))
    base, adv, occupied, scale = call(
        note_kernel,
        [shape(SLOT, 1, dtype=F32)] * 3 + [shape(1, 1, dtype=F32)],
        [VMEM] * 6,
        (
            stats,
            *[shift(stats, "col", COLS, k) for k in range(1, COLS)],
            mine,
            log_normalizer[None, :],
        ),
        flops=4000000,
        size=1 << 18,
    )
    sum_a, sum_b = call(
        add_kernel,
        [shape(*far_a.shape)] * 2,
        [VMEM] * 4,
        (right_a, from_left, left_b, from_right),
        flops=1000000,
        size=3 << 20,
    )
    two_a = shift(sum_a, "mp", SHARDS, 1)
    two_b = shift(sum_b, "mp", SHARDS, -1)

    own = {(0, s): v for s, v in own_first.items()}
    own |= {(1, s): v for s, v in (own_near | own_far).items()}
    names = sorted(own)
    known, factor = call(
        functools.partial(prepare_kernel, names),
        [shape(SLOT, w_out.shape[1], dtype=F32)] * 2,
        [VMEM] * (len(names) + 6),
        (*[own[n] for n in names], own_a, raw_a, own_b, raw_b, last_gain, chosen_rows),
        flops=4000000,
        size=6 << 20,
    )
    objective, totals = call(
        finish_kernel,
        [shape(1, SLOT, dtype=F32), shape(SLOT, 1, SLOT, dtype=F32)],
        [VMEM] * 7,
        (known, factor, two_a, two_b, base, adv, occupied),
        flops=8000000,
        size=6 << 20,
    )
    sums = lax.all_to_all(totals, ROW_COL_MP, 0, 0, tiled=True)
    loss = jnp.sum(sums[:, 0, 0]) * scale[0, 0]
    return objective.reshape(SLOT), loss


def solution(mesh):
    placed = (
        P(ROW_COL, "mp"),
        P(ROW_COL),
        P(ROW_COL),
        P(ROW_COL),
        P(ROW_COL),
        P(ROW_COL),
        P(ROW_COL),
        P(),
        P(None, "mp"),
        P("mp"),
        P(None, "mp"),
        P("mp"),
        P(None, "mp"),
        P("mp"),
        P("mp", None),
        P(),
        P(ROW_COL_MP, None),
        P(ROW_COL_MP),
    )

    return jax.shard_map(
        body, mesh=mesh, in_specs=placed, out_specs=(P(ROW_COL_MP), P()), check_vma=False
    )
```

```python
import functools

import jax
import jax.numpy as jnp
import numpy as np
from jax import lax
from jax.experimental import pallas as pl
from jax.experimental.pallas import tpu as pltpu
from jax.sharding import PartitionSpec as P


HEAD = 128
GROUP_SIZE = 8
SLOT = 128
ROWS = 8
COLS = 4
SHARDS = 4
PACK = 512
ROW_COL = ("row", "col")
ROW_COL_MP = ("row", "col", "mp")
PARTNERS = ((2, 0), (2, 1), (1, 0), (3, 0), (1, 1), (3, 1), (0, 1))
CHUNKS = (384, 512)
STARTS = (0, 384)

norm_eps = 1e-06
rope_theta = 1000000.0
clip_low = 0.2
clip_high = 0.28
std_floor = 1.0
mask_fill = -1e30

F32 = jnp.float32
BF16 = jnp.bfloat16
VMEM = pl.BlockSpec(memory_space=pltpu.VMEM)
SMEM = pl.BlockSpec(memory_space=pltpu.SMEM)
HBM = pl.BlockSpec(memory_space=pltpu.HBM)


def call(kernel, out_shape, in_specs, args, *, flops, size, scratch=(), limit=16 << 20):
    return pl.pallas_call(
        kernel,
        out_shape=out_shape,
        in_specs=in_specs,
        out_specs=jax.tree.map(lambda _: VMEM, out_shape),
        scratch_shapes=list(scratch),
        compiler_params=pltpu.CompilerParams(vmem_limit_bytes=limit),
        cost_estimate=pl.CostEstimate(flops=flops, bytes_accessed=size, transcendentals=0),
    )(*args)


def shape(*dims, dtype=BF16):
    return jax.ShapeDtypeStruct(dims, dtype)


def in_hbm(value):
    return pltpu.with_memory_space_constraint(value, pltpu.HBM)


def across(value, chips, other):
    pairs = [(2 * y + c, 2 * ((y + chips) % 4) + (c ^ other)) for y in range(4) for c in range(2)]
    return lax.ppermute(value, "row", pairs)


def in_vmem(value):
    return pltpu.with_memory_space_constraint(value, pltpu.VMEM)


def shift(value, axis, size, by):
    return lax.ppermute(value, axis, [(i, (i + by) % size) for i in range(size)])


def three_parts(value):
    high = value.astype(BF16).astype(F32)
    middle = (value - high).astype(BF16).astype(F32)
    return high, middle, value - high - middle


def by_row(rows):
    sub = lax.broadcasted_iota(jnp.int32, (8, SLOT), 0)
    tile = jnp.zeros((8, SLOT), F32)
    for n, value in enumerate(rows):
        tile = jnp.where(sub == n, value, tile)
    return tile


def send_kernel(*refs):
    sources, hidden, outs = refs[:6], refs[6], refs[7:-9]
    *held, order, small, sems = refs[-9:]
    row = lax.axis_index("row").astype(jnp.int32)
    loads = [pltpu.make_async_copy(a, b, small.at[i]) for i, (a, b) in enumerate(zip(sources, held))]
    for load in loads:
        load.start()
    for load in loads:
        load.wait()
    dest_of, length_of, offset_of, group_of, reward_of, old_logp = held
    chip, core = lax.shift_right_logical(row, 1), lax.rem(row, 2)
    for slot in range(ROWS):
        to = lax.shift_right_logical(dest_of[slot], 2)
        chips = lax.rem(lax.shift_right_logical(to, 1) - chip + 4, 4)
        order[2 * chips + lax.rem(lax.rem(to, 2) + core, 2)] = slot
    copies = []
    targets = [[(outs[k], 0) for k in range(ROWS)]]
    own, near, other = outs[ROWS:]
    targets.append(
        [
            (own, 0) if k == 0 else (other, k // 2) if k % 2 else (near, k // 2 - 1)
            for k in range(ROWS)
        ]
    )
    for c in range(len(CHUNKS)):
        for k in range(ROWS):
            target, at = targets[c][k]
            copies.append(
                pltpu.make_async_copy(
                    hidden.at[
                        pl.ds(pl.multiple_of(order[k] * SLOT, SLOT), SLOT),
                        pl.ds(STARTS[c], CHUNKS[c]),
                    ],
                    target.at[pl.ds(at * SLOT, SLOT), :],
                    sems.at[c * ROWS + k],
                )
            )
            copies[-1].start()
    lane = lax.broadcasted_iota(jnp.int32, (1, SLOT), 1)
    shared = []
    for entries in (reward_of, group_of, length_of):
        value = jnp.zeros((1, SLOT), F32)
        for i in range(ROWS):
            value = jnp.where(lane == i, entries[i].astype(F32), value)
        shared.append(value)
    for k in range(ROWS):
        slot = order[k]
        place = offset_of[slot]
        high = lax.shift_right_logical(place, 4)
        low = place - high * 16
        own = by_row(
            (
                length_of[slot].astype(F32),
                high.astype(F32),
                low.astype(F32),
                *three_parts(old_logp[pl.ds(slot, 1), :]),
            )
        )
        common = by_row((*three_parts(shared[0]), shared[1], shared[2], slot.astype(F32)))
        outs[k][SLOT : SLOT + 8, 0:SLOT] = own.astype(BF16)
        outs[k][SLOT : SLOT + 8, SLOT : 2 * SLOT] = common.astype(BF16)
        if CHUNKS[0] > 2 * SLOT:
            outs[k][SLOT : SLOT + 8, 2 * SLOT :] = jnp.zeros((8, CHUNKS[0] - 2 * SLOT), BF16)
    for copy in copies:
        copy.wait()


def send_blocks(*args):
    outs = [shape(SLOT + 8, CHUNKS[0])] * ROWS
    outs += [shape(n * SLOT, CHUNKS[1]) for n in (1, 3, 4)]
    flat = call(
        send_kernel,
        outs,
        [HBM] * 7,
        [in_hbm(a) for a in args],
        flops=1000000,
        size=4 << 20,
        scratch=[
            *[pltpu.SMEM((ROWS,), jnp.int32)] * 4,
            pltpu.SMEM((ROWS,), F32),
            pltpu.VMEM((ROWS, SLOT), F32),
            pltpu.SMEM((ROWS,), jnp.int32),
            pltpu.SemaphoreType.DMA((6,)),
            pltpu.SemaphoreType.DMA((2 * ROWS,)),
        ],
    )
    return flat[:ROWS], flat[ROWS:]


def merge_kernel(near, other, *outs):
    for n, out in enumerate(outs):
        out[0:SLOT, :] = near[n * SLOT : (n + 1) * SLOT, :]
        out[SLOT:, :] = other[(n + 1) * SLOT : (n + 2) * SLOT, :]


def settle_kernel(positions, frequency, *refs):
    count = (len(refs) - 3) // 2
    cosine, sine, *held = refs[count:-1]
    copies = [pltpu.make_async_copy(refs[i], held[i], refs[-1].at[i]) for i in range(count)]
    for copy in copies:
        copy.start()
    angle = positions[...] * frequency[...]
    lane = lax.broadcasted_iota(jnp.int32, angle.shape, 1)
    cosine[...] = jnp.cos(angle)
    sine[...] = jnp.where(lane < HEAD // 2, -1.0, 1.0) * jnp.sin(angle)
    for copy in copies:
        copy.wait()


def settle(positions, frequency, *values):
    return call(
        settle_kernel,
        [shape(PACK, HEAD, dtype=F32)] * 2 + [pltpu.VMEM(v.shape, v.dtype) for v in values],
        [VMEM] * 2 + [HBM] * len(values),
        [positions, frequency, *[in_hbm(v) for v in values]],
        flops=1000000,
        size=16 << 20,
        scratch=[pltpu.SemaphoreType.DMA((len(values),))],
    )


def pack_kernel(first, *refs):
    if first:
        blocks = refs[:ROWS]
        upper, lower, positions, notes = refs[ROWS:]
    else:
        own, other, *pairs, notes, upper, lower = refs
        blocks = [own, other, *pairs]
    place = lax.broadcasted_iota(jnp.int32, (PACK, SLOT), 0).astype(F32)
    lane = lax.broadcasted_iota(jnp.int32, (PACK, SLOT), 1).astype(F32)
    picks = []
    within = jnp.zeros((PACK, SLOT), F32)
    for k in range(ROWS):
        if first:
            notes[8 * k : 8 * k + 8, :] = blocks[k][SLOT : SLOT + 8, 0 : 2 * SLOT]
            note = blocks[k][SLOT : SLOT + 8, 0:SLOT].astype(F32)
        else:
            note = notes[8 * k : 8 * k + 8, 0:SLOT].astype(F32)
        length = note[0:1, :]
        offset = note[1:2, :] * 16.0 + note[2:3, :]
        hit = (place - offset == lane) & (lane < length)
        picks.append(jnp.where(hit, 1.0, 0.0).astype(BF16))
        if first:
            within = within + jnp.where(hit, lane, 0.0)
    pick = jnp.concatenate(picks, 1)
    if first:
        rows = jnp.concatenate([b[0:SLOT, :] for b in blocks], 0)
    else:
        rows = jnp.concatenate([own[...], other[0:SLOT, :], *[p[...] for p in pairs]], 0)
    packed = jnp.dot(pick, rows, preferred_element_type=F32).astype(BF16)
    upper[...] = packed[: PACK // 2]
    lower[...] = packed[PACK // 2 :]
    if first:
        positions[...] = jnp.broadcast_to(jnp.sum(within, 1, keepdims=True), (PACK, SLOT))


def pack(c, blocks, notes=None):
    args = list(blocks)
    outs = [shape(PACK // 2, CHUNKS[c])] * 2
    if notes is None:
        outs += [shape(PACK, SLOT, dtype=F32), shape(8 * ROWS, 2 * SLOT)]
    else:
        args.append(notes)
    return call(
        functools.partial(pack_kernel, notes is None),
        outs,
        [VMEM] * len(args),
        args,
        flops=2 * PACK * 8 * SLOT * CHUNKS[c],
        size=2 << 20,
    )


def gather_halves(upper, lower):
    left_upper = shift(upper, "mp", SHARDS, 1)
    left_lower = shift(lower, "mp", SHARDS, 1)
    right_lower = shift(lower, "mp", SHARDS, -1)
    right_upper = shift(upper, "mp", SHARDS, -1)
    far_upper = shift(left_upper, "mp", SHARDS, 1)
    far_lower = shift(right_lower, "mp", SHARDS, -1)
    return {
        0: (upper, lower),
        3: (left_upper, left_lower),
        1: (right_upper, right_lower),
        2: (far_upper, far_lower),
    }


def project_kernel(c, steps, carried, last, *refs):
    width = CHUNKS[c]
    refs = list(refs)
    half = PACK // 2
    halves = [(refs.pop(0), refs.pop(0)) for _ in steps]
    vector, w_query, w_key, w_value = [refs.pop(0) for _ in range(4)]
    if carried:
        total_in, square_in = refs.pop(0), refs.pop(0)
    if last:
        cosine, sine = refs.pop(0), refs.pop(0)
        queries, keys, values = refs.pop(0), refs.pop(0), refs.pop(0)
    else:
        total_out, square_out = refs.pop(0), refs.pop(0)
    own = refs
    me = lax.axis_index("mp").astype(jnp.int32)
    begin = pl.multiple_of(lax.rem(me, 2) * SLOT, SLOT)
    for i, (upper, lower) in enumerate(halves):
        own[i][...] = jnp.where(
            me < 2, upper[pl.ds(begin, SLOT), :], lower[pl.ds(begin, SLOT), :]
        )
    sources = [lax.rem(me + step, SHARDS) for step in steps]
    features = w_query.shape[0] // SHARDS
    picked = [
        pl.ds(pl.multiple_of(source * features + STARTS[c], SLOT), width) for source in sources
    ]

    def weights(i, tile):
        if tile < 3:
            return w_query[picked[i], tile * 256 : tile * 256 + 256]
        if tile == 3:
            return jnp.concatenate([w_query[picked[i], 768:896], w_key[picked[i], :]], 1)
        return w_value[picked[i], :]

    for h in range(2):
        rows = slice(h * half, (h + 1) * half)
        square = jnp.zeros((half, SLOT), F32)
        scaled = []
        for i, pair in enumerate(halves):
            wide = pair[h][...].astype(F32)
            for j in range(0, width, SLOT):
                square = square + wide[:, j : j + SLOT] * wide[:, j : j + SLOT]
            factor = vector[0:1, picked[i]]
            scaled.append((wide * factor).astype(BF16))
        if carried:
            square = square + square_in[rows, :]
        if last:
            mean = jnp.sum(square, 1, keepdims=True) * (1.0 / (SHARDS * features))
            inverse = lax.rsqrt(mean + norm_eps)
            bias = vector[0:1, SHARDS * features :]
        else:
            square_out[rows, :] = square
        for tile in range(5):
            columns = slice(tile * 256, min(tile * 256 + 256, 9 * HEAD))
            part = None
            for i in range(len(steps)):
                term = jnp.dot(scaled[i], weights(i, tile), preferred_element_type=F32)
                part = term if part is None else part + term
            if carried:
                part = part + total_in[rows, columns]
            if not last:
                total_out[rows, columns] = part
                continue
            part = part * inverse + bias[:, columns]
            for n in range(part.shape[1] // HEAD):
                head = part[:, n * HEAD : (n + 1) * HEAD]
                at = 2 * tile + n
                if at < 8:
                    head = head * cosine[rows, :] + pltpu.roll(head, HEAD // 2, 1) * sine[rows, :]
                if at < 7:
                    queries[rows, at * HEAD : (at + 1) * HEAD] = head.astype(BF16)
                elif at == 7:
                    keys[rows, :] = head.astype(BF16)
                else:
                    values[rows, :] = head.astype(BF16)


def project(c, steps, pieces, weights, carried=None, tables=None):
    width = CHUNKS[c]
    columns = 9 * HEAD
    args = []
    for step in steps:
        args += list(pieces[step])
    args += list(weights)
    if carried is not None:
        args += list(carried)
    if tables is None:
        outs = [shape(PACK, columns, dtype=F32), shape(PACK, SLOT, dtype=F32)]
    else:
        args += list(tables)
        outs = [shape(PACK, 7 * HEAD), shape(PACK, HEAD), shape(PACK, HEAD)]
    keep = len(outs)
    outs += [shape(SLOT, width)] * len(steps)
    result = call(
        functools.partial(
            project_kernel, c, steps, carried is not None, tables is not None),
        outs,
        [VMEM] * len(args),
        args,
        flops=2 * PACK * width * len(steps) * columns,
        size=len(steps) * width * (columns + PACK) * 2 + (4 << 20),
    )
    return result[:keep], dict(zip(steps, result[keep:]))


def attend_kernel(steps, queries, keys, values, positions, w_out, *outs):
    me = lax.axis_index("mp").astype(jnp.int32)
    heads = queries.shape[1] // HEAD
    for n, step in enumerate(steps):
        block = lax.rem(me + step, SHARDS)
        begin = pl.multiple_of(block * SLOT, SLOT)
        window = pl.multiple_of(jnp.maximum(block - 1, 0) * SLOT, SLOT)
        row = begin.astype(F32) + lax.broadcasted_iota(jnp.int32, (SLOT, SLOT), 0).astype(F32)
        lane = window.astype(F32) + lax.broadcasted_iota(jnp.int32, (SLOT, SLOT), 1).astype(F32)
        row_start = row - positions[pl.ds(begin, SLOT), :]
        allowed = jnp.concatenate(
            [(lane >= row_start) & (lane <= row), (lane + SLOT >= row_start) & (lane + SLOT <= row)], 1
        )
        all_keys = keys[pl.ds(window, 2 * SLOT), :]
        all_values = values[pl.ds(window, 2 * SLOT), :]
        mixed = []
        for h in range(heads):
            scores = lax.dot_general(
                queries[pl.ds(begin, SLOT), h * HEAD : (h + 1) * HEAD],
                all_keys,
                (((1,), (1,)), ((), ())),
                preferred_element_type=F32,
            )
            scores = jnp.where(allowed, scores * HEAD ** (-0.5), mask_fill)
            exponent = jnp.exp(scores - jnp.max(scores, 1, keepdims=True))
            weights = (exponent * (1.0 / jnp.sum(exponent, 1, keepdims=True))).astype(BF16)
            mixed.append(
                jnp.dot(weights, all_values, preferred_element_type=F32).astype(BF16)
            )
        mixed = jnp.concatenate(mixed, 1)
        for j in range(0, w_out.shape[1], 512):
            part = jnp.dot(mixed, w_out[:, j : j + 512], preferred_element_type=F32).astype(BF16)
            outs[2 * n][:, j : j + 512] = part[: SLOT // 2]
            outs[2 * n + 1][:, j : j + 512] = part[SLOT // 2 :]


def attend(steps, queries, keys, values, positions, w_out):
    width = w_out.shape[1]
    return call(
        functools.partial(attend_kernel, steps),
        [shape(SLOT // 2, width)] * (2 * len(steps)),
        [VMEM] * 5,
        (queries, keys, values, positions, w_out),
        flops=len(steps) * 2 * SLOT * w_out.shape[0] * (width + 4 * SLOT),
        size=8 << 20,
    )


def add_kernel(a, b, c, d, ab, cd):
    ab[...] = (a[...].astype(F32) + b[...].astype(F32)).astype(BF16)
    cd[...] = (c[...].astype(F32) + d[...].astype(F32)).astype(BF16)


def sort_kernel(notes, stats_out, mine_out):
    lane = lax.broadcasted_iota(jnp.int32, (1, SLOT), 1)
    for k in range(ROWS):
        own = notes[8 * k : 8 * k + 8, 0:SLOT].astype(F32)
        common = notes[8 * k : 8 * k + 8, SLOT : 2 * SLOT].astype(F32)
        rewards = common[0:1, :] + common[1:2, :] + common[2:3, :]
        groups = common[3:4, :]
        picked = lane.astype(F32) == common[5:6, :]
        stats_out[k : k + 1, :] = (
            rewards + pltpu.roll(groups, 8, 1) + pltpu.roll(common[4:5, :], 16, 1)
        )
        info = jnp.where(lane == 26, own[1:2, :] * 16.0 + own[2:3, :], 0.0)
        info = jnp.where(lane == 27, own[0:1, :], info)
        for n, value in ((24, rewards), (25, groups)):
            info = jnp.where(
                lane == n, jnp.sum(jnp.where(picked, value, 0.0), 1, keepdims=True), info
            )
        mine_out[k : k + 1, 0:SLOT] = own[3:4, :] + own[4:5, :] + own[5:6, :]
        mine_out[k : k + 1, SLOT:] = info


def note_kernel(stats_a, stats_b, stats_c, stats_d, mine_ref, log_normalizer, base_out, adv_out, occupied_out, scale_out):
    me = lax.axis_index("mp").astype(jnp.int32)
    lane32 = lax.broadcasted_iota(jnp.int32, (COLS * ROWS, SLOT), 1)
    rewards = jnp.concatenate([stats_a[...], stats_b[...], stats_c[...], stats_d[...]], 0)
    groups = pltpu.roll(rewards, SLOT - 8, 1)
    lengths = pltpu.roll(rewards, SLOT - 16, 1)
    valid = lane32 < 8
    place = (lax.broadcasted_iota(jnp.int32, (SLOT, SLOT), 0) + me * SLOT).astype(F32)
    lane_int = lax.broadcasted_iota(jnp.int32, (SLOT, SLOT), 1)
    lane = lane_int.astype(F32)
    one_lane = lax.broadcasted_iota(jnp.int32, (1, SLOT), 1)

    def total(value):
        return jnp.sum(jnp.sum(value, 1, keepdims=True), 0, keepdims=True)

    old = jnp.zeros((SLOT, SLOT), F32)
    adv = jnp.zeros((SLOT, SLOT), F32)
    occupied = jnp.zeros((SLOT, SLOT), F32)
    for r in range(ROWS):
        mine = mine_ref[r : r + 1, :]
        info = mine[:, SLOT:]

        def entry(at):
            return jnp.sum(jnp.where(one_lane == at, info, 0.0), 1, keepdims=True)

        reward, group, offset, length = entry(24), entry(25), entry(26), entry(27)
        member = valid & (groups == group)
        mean = total(jnp.where(member, rewards, 0.0)) / GROUP_SIZE
        centered = jnp.where(member, rewards - mean, 0.0)
        spread = total(centered * centered) / GROUP_SIZE
        advantage = (reward - mean) / jnp.maximum(jnp.sqrt(spread), std_floor)
        hit = (place - offset == lane) & (lane < length)
        old = old + jnp.where(hit, mine[:, :SLOT], 0.0)
        adv = adv + jnp.where(hit, advantage, 0.0)
        occupied = occupied + jnp.where(hit, 1.0, 0.0)
    diagonal = lane_int == lax.broadcasted_iota(jnp.int32, (SLOT, SLOT), 0)
    old = old + jnp.where(diagonal, log_normalizer[...], 0.0)
    base_out[...] = jnp.sum(old, 1, keepdims=True)
    adv_out[...] = jnp.sum(adv, 1, keepdims=True)
    occupied_out[...] = jnp.sum(occupied, 1, keepdims=True)
    scale_out[...] = -1.0 / total(jnp.where(valid, lengths, 0.0))


def prepare_kernel(keys, *refs):
    refs = list(refs)
    own = [refs.pop(0) for _ in keys]
    own_a, raw_a, own_b, raw_b, gain, chosen, known, factor = refs
    me = lax.axis_index("mp").astype(jnp.int32)
    for (c, step), resid in zip(keys, own):
        start = lax.rem(me + step, SHARDS) * sum(CHUNKS) + STARTS[c]
        for j in range(0, CHUNKS[c], SLOT):
            at = pl.ds(pl.multiple_of(start + j, SLOT), SLOT)
            branch = jnp.concatenate(
                [
                    own_a[:, at].astype(F32) + raw_a[:, at].astype(F32),
                    own_b[:, at].astype(F32) + raw_b[:, at].astype(F32),
                ],
                0,
            )
            known[:, at] = resid[:, j : j + SLOT].astype(F32) + branch
    factor[...] = gain[...].astype(F32) * chosen[...].astype(F32)


def finish_kernel(known, factor, two_a, two_b, base, adv, occupied, objective_out, total_out):
    width = known.shape[1]
    square = jnp.zeros((SLOT, SLOT), F32)
    product = jnp.zeros((SLOT, SLOT), F32)
    for j in range(0, width, SLOT):
        at = slice(j, j + SLOT)
        two = jnp.concatenate([two_a[:, at].astype(F32), two_b[:, at].astype(F32)], 0)
        rows = (known[:, at] + two).astype(BF16).astype(F32)
        square = square + rows * rows
        product = product + rows * factor[:, at]
    mean = jnp.sum(square, 1, keepdims=True) * (1.0 / width)
    logits = jnp.sum(product, 1, keepdims=True) * lax.rsqrt(mean + norm_eps)
    ratios = jnp.exp(logits - base[...])
    bounded = jnp.clip(ratios, 1.0 - clip_low, 1.0 + clip_high)
    value = jnp.minimum(ratios * adv[...], bounded * adv[...])
    value = jnp.where(occupied[...] > 0.5, value, 0.0)
    diagonal = lax.broadcasted_iota(jnp.int32, (SLOT, SLOT), 1) == lax.broadcasted_iota(
        jnp.int32, (SLOT, SLOT), 0
    )
    line = jnp.sum(jnp.where(diagonal, value, 0.0), 0, keepdims=True)
    objective_out[...] = line
    total = jnp.sum(line, 1, keepdims=True)
    total_out[...] = jnp.broadcast_to(total[None], (SLOT, 1, SLOT))


def body(
    hidden,
    old_logp,
    rewards,
    resp_dest,
    resp_len,
    resp_offset,
    prompt_group,
    attn_gain,
    w_query,
    q_bias,
    w_key,
    k_bias,
    w_value,
    v_bias,
    w_out,
    final_gain,
    chosen_rows,
    log_normalizer,
):
    blocks, later = send_blocks(
        resp_dest,
        resp_len,
        resp_offset,
        prompt_group,
        rewards,
        old_logp.reshape(ROWS, SLOT),
        hidden,
    )
    first_blocks = [blocks[0]] + [None] * (ROWS - 1)
    for chips, other in PARTNERS:
        at = 2 * chips + other
        first_blocks[at] = across(blocks[at], chips, other)
    own_block, near_blocks, other_blocks = later
    from_other = across(other_blocks, 0, 1)
    merged = call(
        merge_kernel,
        [shape(2 * SLOT, CHUNKS[1])] * 3,
        [VMEM] * 2,
        (near_blocks, from_other),
        flops=100000,
        size=1 << 20,
    )
    pairs = [None] * 3
    for chips in (1, 3, 2):
        pairs[chips - 1] = across(merged[chips - 1], chips, 0)

    vector = jnp.concatenate([v.astype(F32) for v in (attn_gain, q_bias, k_bias, v_bias)])[None, :]
    exponents = (np.arange(HEAD) % (HEAD // 2)) * (2.0 / HEAD)
    frequency = jnp.asarray((rope_theta ** (-exponents))[None, :], F32)
    first_blocks[0], vector = lax.optimization_barrier((first_blocks[0], vector))
    upper, lower, positions, notes = pack(0, first_blocks)
    first = gather_halves(upper, lower)
    second = gather_halves(*pack(1, [own_block, from_other, *pairs], notes))
    cosine, sine, *held = settle(positions, frequency, w_query, w_key, w_value, w_out)
    *weights, w_out = [in_vmem(v) for v in held]
    weights = (vector, *weights)
    tables = (cosine, sine)
    carried, own_first = project(0, (0, 1, 3, 2), first, weights)
    carried, own_near = project(1, (0, 1, 3), second, weights, carried)
    (queries, keys, values), own_far = project(1, (2,), second, weights, carried, tables)

    attend_to = functools.partial(
        attend,
        queries=queries,
        keys=keys,
        values=values,
        positions=positions,
        w_out=w_out,
    )
    far_a, far_b = attend_to((2,))
    from_left = shift(far_a, "mp", SHARDS, 1)
    from_right = shift(far_b, "mp", SHARDS, -1)
    right_a, right_b, left_a, left_b = attend_to((1, 3))
    raw_b = shift(right_b, "mp", SHARDS, 1)
    raw_a = shift(left_a, "mp", SHARDS, -1)
    notes, left_b = lax.optimization_barrier((notes, left_b))
    stats, mine = call(
        sort_kernel,
        [shape(ROWS, SLOT, dtype=F32), shape(ROWS, 2 * SLOT, dtype=F32)],
        [VMEM],
        (notes,),
        flops=100000,
        size=1 << 17,
    )
    base, adv, occupied, scale = call(
        note_kernel,
        [shape(SLOT, 1, dtype=F32)] * 3 + [shape(1, 1, dtype=F32)],
        [VMEM] * 6,
        (
            stats,
            *[shift(stats, "col", COLS, k) for k in range(1, COLS)],
            mine,
            log_normalizer[None, :],
        ),
        flops=4000000,
        size=1 << 18,
    )
    sum_a, sum_b = call(
        add_kernel,
        [shape(*far_a.shape)] * 2,
        [VMEM] * 4,
        (right_a, from_left, left_b, from_right),
        flops=1000000,
        size=3 << 20,
    )
    two_a = shift(sum_a, "mp", SHARDS, 1)
    two_b = shift(sum_b, "mp", SHARDS, -1)
    own_a, own_b = attend_to((0,))
    final_gain, own_a = lax.optimization_barrier((final_gain, own_a))
    last_gain = final_gain[None, :]

    own = {(0, s): v for s, v in own_first.items()}
    own |= {(1, s): v for s, v in (own_near | own_far).items()}
    names = sorted(own)
    known, factor = call(
        functools.partial(prepare_kernel, names),
        [shape(SLOT, w_out.shape[1], dtype=F32)] * 2,
        [VMEM] * (len(names) + 6),
        (*[own[n] for n in names], own_a, raw_a, own_b, raw_b, last_gain, chosen_rows),
        flops=4000000,
        size=6 << 20,
    )
    objective, totals = call(
        finish_kernel,
        [shape(1, SLOT, dtype=F32), shape(SLOT, 1, SLOT, dtype=F32)],
        [VMEM] * 7,
        (known, factor, two_a, two_b, base, adv, occupied),
        flops=8000000,
        size=6 << 20,
    )
    sums = lax.all_to_all(totals, ROW_COL_MP, 0, 0, tiled=True)
    loss = jnp.sum(sums[:, 0, 0]) * scale[0, 0]
    return objective.reshape(SLOT), loss


def solution(mesh):
    placed = (
        P(ROW_COL, "mp"),
        P(ROW_COL),
        P(ROW_COL),
        P(ROW_COL),
        P(ROW_COL),
        P(ROW_COL),
        P(ROW_COL),
        P(),
        P(None, "mp"),
        P("mp"),
        P(None, "mp"),
        P("mp"),
        P(None, "mp"),
        P("mp"),
        P("mp", None),
        P(),
        P(ROW_COL_MP, None),
        P(ROW_COL_MP),
    )

    return jax.shard_map(
        body, mesh=mesh, in_specs=placed, out_specs=(P(ROW_COL_MP), P()), check_vma=False
    )
```

```python
import functools

import jax
import jax.numpy as jnp
import numpy as np
from jax import lax
from jax.experimental import pallas as pl
from jax.experimental.pallas import tpu as pltpu
from jax.sharding import PartitionSpec as P


HEAD = 128
GROUP_SIZE = 8
SLOT = 128
ROWS = 8
COLS = 4
SHARDS = 4
PACK = 512
ROW_COL = ("row", "col")
ROW_COL_MP = ("row", "col", "mp")
PARTNERS = ((2, 0), (2, 1), (1, 0), (3, 0), (1, 1), (3, 1), (0, 1))
CHUNKS = (384, 512)
STARTS = (0, 384)

norm_eps = 1e-06
rope_theta = 1000000.0
clip_low = 0.2
clip_high = 0.28
std_floor = 1.0
mask_fill = -1e30

F32 = jnp.float32
BF16 = jnp.bfloat16
VMEM = pl.BlockSpec(memory_space=pltpu.VMEM)
SMEM = pl.BlockSpec(memory_space=pltpu.SMEM)
HBM = pl.BlockSpec(memory_space=pltpu.HBM)


def call(kernel, out_shape, in_specs, args, *, flops, size, scratch=(), limit=16 << 20):
    return pl.pallas_call(
        kernel,
        out_shape=out_shape,
        in_specs=in_specs,
        out_specs=jax.tree.map(lambda _: VMEM, out_shape),
        scratch_shapes=list(scratch),
        compiler_params=pltpu.CompilerParams(vmem_limit_bytes=limit),
        cost_estimate=pl.CostEstimate(flops=flops, bytes_accessed=size, transcendentals=0),
    )(*args)


def shape(*dims, dtype=BF16):
    return jax.ShapeDtypeStruct(dims, dtype)


def in_hbm(value):
    return pltpu.with_memory_space_constraint(value, pltpu.HBM)


def across(value, chips, other):
    pairs = [(2 * y + c, 2 * ((y + chips) % 4) + (c ^ other)) for y in range(4) for c in range(2)]
    return lax.ppermute(value, "row", pairs)


def in_vmem(value):
    return pltpu.with_memory_space_constraint(value, pltpu.VMEM)


def shift(value, axis, size, by):
    return lax.ppermute(value, axis, [(i, (i + by) % size) for i in range(size)])


def three_parts(value):
    high = value.astype(BF16).astype(F32)
    middle = (value - high).astype(BF16).astype(F32)
    return high, middle, value - high - middle


def by_row(rows):
    sub = lax.broadcasted_iota(jnp.int32, (8, SLOT), 0)
    tile = jnp.zeros((8, SLOT), F32)
    for n, value in enumerate(rows):
        tile = jnp.where(sub == n, value, tile)
    return tile


def send_kernel(*refs):
    sources, hidden, outs = refs[:6], refs[6], refs[7:-10]
    *held, order, rows_held, small, sems = refs[-10:]
    row = lax.axis_index("row").astype(jnp.int32)
    loads = [pltpu.make_async_copy(a, b, small.at[i]) for i, (a, b) in enumerate(zip(sources, held))]
    for load in loads:
        load.start()
    copies = [
        pltpu.make_async_copy(
            hidden.at[pl.ds(n * SLOT, SLOT), :], rows_held.at[pl.ds(n * SLOT, SLOT), :], sems.at[n]
        )
        for n in range(ROWS)
    ]
    for copy in copies:
        copy.start()
    for load in loads:
        load.wait()
    dest_of, length_of, offset_of, group_of, reward_of, old_logp = held
    chip, core = lax.shift_right_logical(row, 1), lax.rem(row, 2)
    for slot in range(ROWS):
        to = lax.shift_right_logical(dest_of[slot], 2)
        chips = lax.rem(lax.shift_right_logical(to, 1) - chip + 4, 4)
        order[2 * chips + lax.rem(lax.rem(to, 2) + core, 2)] = slot
    lane = lax.broadcasted_iota(jnp.int32, (1, SLOT), 1)
    shared = []
    for entries in (reward_of, group_of, length_of):
        value = jnp.zeros((1, SLOT), F32)
        for i in range(ROWS):
            value = jnp.where(lane == i, entries[i].astype(F32), value)
        shared.append(value)
    for k in range(ROWS):
        slot = order[k]
        place = offset_of[slot]
        high = lax.shift_right_logical(place, 4)
        low = place - high * 16
        own = by_row(
            (
                length_of[slot].astype(F32),
                high.astype(F32),
                low.astype(F32),
                *three_parts(old_logp[pl.ds(slot, 1), :]),
            )
        )
        common = by_row((*three_parts(shared[0]), shared[1], shared[2], slot.astype(F32)))
        outs[k][SLOT : SLOT + 8, 0:SLOT] = own.astype(BF16)
        outs[k][SLOT : SLOT + 8, SLOT : 2 * SLOT] = common.astype(BF16)
        if CHUNKS[0] > 2 * SLOT:
            outs[k][SLOT : SLOT + 8, 2 * SLOT :] = jnp.zeros((8, CHUNKS[0] - 2 * SLOT), BF16)
    for copy in copies:
        copy.wait()
    own, near, other = outs[ROWS:]
    for k in range(ROWS):
        block = rows_held[pl.ds(pl.multiple_of(order[k] * SLOT, SLOT), SLOT), :]
        outs[k][0:SLOT, :] = block[:, : CHUNKS[0]]
        target, at = (own, 0) if k == 0 else (other, k // 2) if k % 2 else (near, k // 2 - 1)
        target[at * SLOT : (at + 1) * SLOT, :] = block[:, CHUNKS[0] :]


def send_blocks(*args):
    outs = [shape(SLOT + 8, CHUNKS[0])] * ROWS
    outs += [shape(n * SLOT, CHUNKS[1]) for n in (1, 3, 4)]
    flat = call(
        send_kernel,
        outs,
        [HBM] * 7,
        [in_hbm(a) for a in args],
        flops=1000000,
        size=4 << 20,
        scratch=[
            *[pltpu.SMEM((ROWS,), jnp.int32)] * 4,
            pltpu.SMEM((ROWS,), F32),
            pltpu.VMEM((ROWS, SLOT), F32),
            pltpu.SMEM((ROWS,), jnp.int32),
            pltpu.VMEM((ROWS * SLOT, sum(CHUNKS)), BF16),
            pltpu.SemaphoreType.DMA((6,)),
            pltpu.SemaphoreType.DMA((ROWS,)),
        ],
    )
    return flat[:ROWS], flat[ROWS:]


def merge_kernel(near, other, *outs):
    for n, out in enumerate(outs):
        out[0:SLOT, :] = near[n * SLOT : (n + 1) * SLOT, :]
        out[SLOT:, :] = other[(n + 1) * SLOT : (n + 2) * SLOT, :]


def settle_kernel(positions, frequency, *refs):
    count = (len(refs) - 3) // 2
    cosine, sine, *held = refs[count:-1]
    copies = [pltpu.make_async_copy(refs[i], held[i], refs[-1].at[i]) for i in range(count)]
    for copy in copies:
        copy.start()
    angle = positions[...] * frequency[...]
    lane = lax.broadcasted_iota(jnp.int32, angle.shape, 1)
    cosine[...] = jnp.cos(angle)
    sine[...] = jnp.where(lane < HEAD // 2, -1.0, 1.0) * jnp.sin(angle)
    for copy in copies:
        copy.wait()


def settle(positions, frequency, *values):
    return call(
        settle_kernel,
        [shape(PACK, HEAD, dtype=F32)] * 2 + [pltpu.VMEM(v.shape, v.dtype) for v in values],
        [VMEM] * 2 + [HBM] * len(values),
        [positions, frequency, *[in_hbm(v) for v in values]],
        flops=1000000,
        size=16 << 20,
        scratch=[pltpu.SemaphoreType.DMA((len(values),))],
    )


def pack_kernel(first, *refs):
    if first:
        blocks = refs[:ROWS]
        upper, lower, positions, notes = refs[ROWS:]
    else:
        own, other, *pairs, notes, upper, lower = refs
        blocks = [own, other, *pairs]
    place = lax.broadcasted_iota(jnp.int32, (PACK, SLOT), 0).astype(F32)
    lane = lax.broadcasted_iota(jnp.int32, (PACK, SLOT), 1).astype(F32)
    picks = []
    within = jnp.zeros((PACK, SLOT), F32)
    for k in range(ROWS):
        if first:
            notes[8 * k : 8 * k + 8, :] = blocks[k][SLOT : SLOT + 8, 0 : 2 * SLOT]
            note = blocks[k][SLOT : SLOT + 8, 0:SLOT].astype(F32)
        else:
            note = notes[8 * k : 8 * k + 8, 0:SLOT].astype(F32)
        length = note[0:1, :]
        offset = note[1:2, :] * 16.0 + note[2:3, :]
        hit = (place - offset == lane) & (lane < length)
        picks.append(jnp.where(hit, 1.0, 0.0).astype(BF16))
        if first:
            within = within + jnp.where(hit, lane, 0.0)
    pick = jnp.concatenate(picks, 1)
    if first:
        rows = jnp.concatenate([b[0:SLOT, :] for b in blocks], 0)
    else:
        rows = jnp.concatenate([own[...], other[0:SLOT, :], *[p[...] for p in pairs]], 0)
    packed = jnp.dot(pick, rows, preferred_element_type=F32).astype(BF16)
    upper[...] = packed[: PACK // 2]
    lower[...] = packed[PACK // 2 :]
    if first:
        positions[...] = jnp.broadcast_to(jnp.sum(within, 1, keepdims=True), (PACK, SLOT))


def pack(c, blocks, notes=None):
    args = list(blocks)
    outs = [shape(PACK // 2, CHUNKS[c])] * 2
    if notes is None:
        outs += [shape(PACK, SLOT, dtype=F32), shape(8 * ROWS, 2 * SLOT)]
    else:
        args.append(notes)
    return call(
        functools.partial(pack_kernel, notes is None),
        outs,
        [VMEM] * len(args),
        args,
        flops=2 * PACK * 8 * SLOT * CHUNKS[c],
        size=2 << 20,
    )


def gather_halves(upper, lower):
    left_upper = shift(upper, "mp", SHARDS, 1)
    left_lower = shift(lower, "mp", SHARDS, 1)
    right_lower = shift(lower, "mp", SHARDS, -1)
    right_upper = shift(upper, "mp", SHARDS, -1)
    far_upper = shift(left_upper, "mp", SHARDS, 1)
    far_lower = shift(right_lower, "mp", SHARDS, -1)
    return {
        0: (upper, lower),
        3: (left_upper, left_lower),
        1: (right_upper, right_lower),
        2: (far_upper, far_lower),
    }


def project_kernel(c, steps, carried, last, *refs):
    width = CHUNKS[c]
    refs = list(refs)
    half = PACK // 2
    halves = [(refs.pop(0), refs.pop(0)) for _ in steps]
    vector, w_query, w_key, w_value = [refs.pop(0) for _ in range(4)]
    if carried:
        total_in, square_in = refs.pop(0), refs.pop(0)
    if last:
        cosine, sine = refs.pop(0), refs.pop(0)
        queries, keys, values = refs.pop(0), refs.pop(0), refs.pop(0)
    else:
        total_out, square_out = refs.pop(0), refs.pop(0)
    own = refs
    me = lax.axis_index("mp").astype(jnp.int32)
    begin = pl.multiple_of(lax.rem(me, 2) * SLOT, SLOT)
    for i, (upper, lower) in enumerate(halves):
        own[i][...] = jnp.where(
            me < 2, upper[pl.ds(begin, SLOT), :], lower[pl.ds(begin, SLOT), :]
        )
    sources = [lax.rem(me + step, SHARDS) for step in steps]
    features = w_query.shape[0] // SHARDS
    picked = [
        pl.ds(pl.multiple_of(source * features + STARTS[c], SLOT), width) for source in sources
    ]

    def weights(i, tile):
        if tile < 3:
            return w_query[picked[i], tile * 256 : tile * 256 + 256]
        if tile == 3:
            return jnp.concatenate([w_query[picked[i], 768:896], w_key[picked[i], :]], 1)
        return w_value[picked[i], :]

    for h in range(2):
        rows = slice(h * half, (h + 1) * half)
        square = jnp.zeros((half, SLOT), F32)
        scaled = []
        for i, pair in enumerate(halves):
            wide = pair[h][...].astype(F32)
            for j in range(0, width, SLOT):
                square = square + wide[:, j : j + SLOT] * wide[:, j : j + SLOT]
            factor = vector[0:1, picked[i]]
            scaled.append((wide * factor).astype(BF16))
        if carried:
            square = square + square_in[rows, :]
        if last:
            mean = jnp.sum(square, 1, keepdims=True) * (1.0 / (SHARDS * features))
            inverse = lax.rsqrt(mean + norm_eps)
            bias = vector[0:1, SHARDS * features :]
        else:
            square_out[rows, :] = square
        for tile in range(5):
            columns = slice(tile * 256, min(tile * 256 + 256, 9 * HEAD))
            part = None
            for i in range(len(steps)):
                term = jnp.dot(scaled[i], weights(i, tile), preferred_element_type=F32)
                part = term if part is None else part + term
            if carried:
                part = part + total_in[rows, columns]
            if not last:
                total_out[rows, columns] = part
                continue
            part = part * inverse + bias[:, columns]
            for n in range(part.shape[1] // HEAD):
                head = part[:, n * HEAD : (n + 1) * HEAD]
                at = 2 * tile + n
                if at < 8:
                    head = head * cosine[rows, :] + pltpu.roll(head, HEAD // 2, 1) * sine[rows, :]
                if at < 7:
                    queries[rows, at * HEAD : (at + 1) * HEAD] = head.astype(BF16)
                elif at == 7:
                    keys[rows, :] = head.astype(BF16)
                else:
                    values[rows, :] = head.astype(BF16)


def project(c, steps, pieces, weights, carried=None, tables=None):
    width = CHUNKS[c]
    columns = 9 * HEAD
    args = []
    for step in steps:
        args += list(pieces[step])
    args += list(weights)
    if carried is not None:
        args += list(carried)
    if tables is None:
        outs = [shape(PACK, columns, dtype=F32), shape(PACK, SLOT, dtype=F32)]
    else:
        args += list(tables)
        outs = [shape(PACK, 7 * HEAD), shape(PACK, HEAD), shape(PACK, HEAD)]
    keep = len(outs)
    outs += [shape(SLOT, width)] * len(steps)
    result = call(
        functools.partial(
            project_kernel, c, steps, carried is not None, tables is not None),
        outs,
        [VMEM] * len(args),
        args,
        flops=2 * PACK * width * len(steps) * columns,
        size=len(steps) * width * (columns + PACK) * 2 + (4 << 20),
    )
    return result[:keep], dict(zip(steps, result[keep:]))


def attend_block(block, heads, all_keys, all_values, positions, w_out, out_a, out_b):
    begin = pl.multiple_of(block * SLOT, SLOT)
    window = jnp.maximum(block - 1, 0) * SLOT
    row = begin.astype(F32) + lax.broadcasted_iota(jnp.int32, (SLOT, SLOT), 0).astype(F32)
    lane = window.astype(F32) + lax.broadcasted_iota(jnp.int32, (SLOT, SLOT), 1).astype(F32)
    row_start = row - positions[pl.ds(begin, SLOT), :]
    allowed = jnp.concatenate(
        [(lane >= row_start) & (lane <= row), (lane + SLOT >= row_start) & (lane + SLOT <= row)], 1
    )
    mixed = []
    for head in heads:
        scores = lax.dot_general(
            head, all_keys, (((1,), (1,)), ((), ())), preferred_element_type=F32
        )
        scores = jnp.where(allowed, scores * HEAD ** (-0.5), mask_fill)
        exponent = jnp.exp(scores - jnp.max(scores, 1, keepdims=True))
        weights = (exponent * (1.0 / jnp.sum(exponent, 1, keepdims=True))).astype(BF16)
        mixed.append(jnp.dot(weights, all_values, preferred_element_type=F32).astype(BF16))
    mixed = jnp.concatenate(mixed, 1)
    for j in range(0, w_out.shape[1], 512):
        part = jnp.dot(mixed, w_out[:, j : j + 512], preferred_element_type=F32).astype(BF16)
        out_a[:, j : j + 512] = part[: SLOT // 2]
        out_b[:, j : j + 512] = part[SLOT // 2 :]


def attend_kernel(steps, queries, keys, values, positions, w_out, *outs):
    me = lax.axis_index("mp").astype(jnp.int32)
    for n, step in enumerate(steps):
        block = lax.rem(me + step, SHARDS)
        begin = pl.multiple_of(block * SLOT, SLOT)
        window = pl.multiple_of(jnp.maximum(block - 1, 0) * SLOT, SLOT)
        attend_block(
            block,
            [
                queries[pl.ds(begin, SLOT), h : h + HEAD]
                for h in range(0, queries.shape[1], HEAD)
            ],
            keys[pl.ds(window, 2 * SLOT), :],
            values[pl.ds(window, 2 * SLOT), :],
            positions,
            w_out,
            outs[2 * n],
            outs[2 * n + 1],
        )


def far_kernel(
    c, upper, lower, vector, w_query, w_key, w_value, total_in, square_in, cosine, sine, positions, w_out, out_a, out_b
):
    me = lax.axis_index("mp").astype(jnp.int32)
    features = w_query.shape[0] // SHARDS
    source = block = lax.rem(me + 2, SHARDS)
    before = jnp.maximum(block - 1, 0)
    picked = pl.ds(pl.multiple_of(source * features + STARTS[c], SLOT), CHUNKS[c])
    factor = vector[0:1, picked]
    bias = vector[0:1, SHARDS * features :]

    def rows_of(at):
        inside = pl.ds(pl.multiple_of(lax.rem(at, 2) * SLOT, SLOT), SLOT)
        return jnp.where(at < 2, upper[inside, :], lower[inside, :])

    def prepared(blocks):
        scaled, inverse = [], []
        for at in blocks:
            wide = rows_of(at).astype(F32)
            square = square_in[pl.ds(pl.multiple_of(at * SLOT, SLOT), SLOT), :]
            for j in range(0, CHUNKS[c], SLOT):
                square = square + wide[:, j : j + SLOT] * wide[:, j : j + SLOT]
            mean = jnp.sum(square, 1, keepdims=True) * (1.0 / (SHARDS * features))
            inverse.append(lax.rsqrt(mean + norm_eps))
            scaled.append((wide * factor).astype(BF16))
        return jnp.concatenate(scaled, 0), jnp.concatenate(inverse, 0)

    def turned(head, rows):
        return (head * cosine[rows, :] + pltpu.roll(head, HEAD // 2, 1) * sine[rows, :]).astype(BF16)

    rows = pl.ds(pl.multiple_of(before * SLOT, SLOT), 2 * SLOT)
    scaled, inverse = prepared([before, before + 1])
    both = jnp.dot(
        scaled,
        jnp.concatenate([w_key[picked, :], w_value[picked, :]], 1),
        preferred_element_type=F32,
    )
    both = (both + total_in[rows, 7 * HEAD :]) * inverse + bias[:, 7 * HEAD :]
    keys = turned(both[:, :HEAD], rows)
    values = both[:, HEAD:].astype(BF16)
    rows = pl.ds(pl.multiple_of(block * SLOT, SLOT), SLOT)
    scaled, inverse = prepared([block])
    heads = []
    for j in range(0, 7 * HEAD, 256):
        columns = slice(j, min(j + 256, 7 * HEAD))
        part = jnp.dot(scaled, w_query[picked, columns], preferred_element_type=F32)
        part = (part + total_in[rows, columns]) * inverse + bias[:, columns]
        heads += [turned(part[:, n : n + HEAD], rows) for n in range(0, part.shape[1], HEAD)]
    attend_block(block, heads, keys, values, positions, w_out, out_a, out_b)


def attend(steps, queries, keys, values, positions, w_out):
    width = w_out.shape[1]
    return call(
        functools.partial(attend_kernel, steps),
        [shape(SLOT // 2, width)] * (2 * len(steps)),
        [VMEM] * 5,
        (queries, keys, values, positions, w_out),
        flops=len(steps) * 2 * SLOT * w_out.shape[0] * (width + 4 * SLOT),
        size=8 << 20,
    )


def add_kernel(a, b, c, d, ab, cd):
    ab[...] = (a[...].astype(F32) + b[...].astype(F32)).astype(BF16)
    cd[...] = (c[...].astype(F32) + d[...].astype(F32)).astype(BF16)


def sort_kernel(notes, stats_out, mine_out):
    lane = lax.broadcasted_iota(jnp.int32, (1, SLOT), 1)
    for k in range(ROWS):
        own = notes[8 * k : 8 * k + 8, 0:SLOT].astype(F32)
        common = notes[8 * k : 8 * k + 8, SLOT : 2 * SLOT].astype(F32)
        rewards = common[0:1, :] + common[1:2, :] + common[2:3, :]
        groups = common[3:4, :]
        picked = lane.astype(F32) == common[5:6, :]
        stats_out[k : k + 1, :] = (
            rewards + pltpu.roll(groups, 8, 1) + pltpu.roll(common[4:5, :], 16, 1)
        )
        info = jnp.where(lane == 26, own[1:2, :] * 16.0 + own[2:3, :], 0.0)
        info = jnp.where(lane == 27, own[0:1, :], info)
        for n, value in ((24, rewards), (25, groups)):
            info = jnp.where(
                lane == n, jnp.sum(jnp.where(picked, value, 0.0), 1, keepdims=True), info
            )
        mine_out[k : k + 1, 0:SLOT] = own[3:4, :] + own[4:5, :] + own[5:6, :]
        mine_out[k : k + 1, SLOT:] = info


def note_kernel(stats_a, stats_b, stats_c, stats_d, mine_ref, log_normalizer, base_out, adv_out, occupied_out, scale_out):
    me = lax.axis_index("mp").astype(jnp.int32)
    lane32 = lax.broadcasted_iota(jnp.int32, (COLS * ROWS, SLOT), 1)
    rewards = jnp.concatenate([stats_a[...], stats_b[...], stats_c[...], stats_d[...]], 0)
    groups = pltpu.roll(rewards, SLOT - 8, 1)
    lengths = pltpu.roll(rewards, SLOT - 16, 1)
    valid = lane32 < 8
    place = (lax.broadcasted_iota(jnp.int32, (SLOT, SLOT), 0) + me * SLOT).astype(F32)
    lane_int = lax.broadcasted_iota(jnp.int32, (SLOT, SLOT), 1)
    lane = lane_int.astype(F32)
    one_lane = lax.broadcasted_iota(jnp.int32, (1, SLOT), 1)

    def total(value):
        return jnp.sum(jnp.sum(value, 1, keepdims=True), 0, keepdims=True)

    old = jnp.zeros((SLOT, SLOT), F32)
    adv = jnp.zeros((SLOT, SLOT), F32)
    occupied = jnp.zeros((SLOT, SLOT), F32)
    for r in range(ROWS):
        mine = mine_ref[r : r + 1, :]
        info = mine[:, SLOT:]

        def entry(at):
            return jnp.sum(jnp.where(one_lane == at, info, 0.0), 1, keepdims=True)

        reward, group, offset, length = entry(24), entry(25), entry(26), entry(27)
        member = valid & (groups == group)
        mean = total(jnp.where(member, rewards, 0.0)) / GROUP_SIZE
        centered = jnp.where(member, rewards - mean, 0.0)
        spread = total(centered * centered) / GROUP_SIZE
        advantage = (reward - mean) / jnp.maximum(jnp.sqrt(spread), std_floor)
        hit = (place - offset == lane) & (lane < length)
        old = old + jnp.where(hit, mine[:, :SLOT], 0.0)
        adv = adv + jnp.where(hit, advantage, 0.0)
        occupied = occupied + jnp.where(hit, 1.0, 0.0)
    diagonal = lane_int == lax.broadcasted_iota(jnp.int32, (SLOT, SLOT), 0)
    old = old + jnp.where(diagonal, log_normalizer[...], 0.0)
    base_out[...] = jnp.sum(old, 1, keepdims=True)
    adv_out[...] = jnp.sum(adv, 1, keepdims=True)
    occupied_out[...] = jnp.sum(occupied, 1, keepdims=True)
    scale_out[...] = -1.0 / total(jnp.where(valid, lengths, 0.0))


def prepare_kernel(keys, *refs):
    refs = list(refs)
    own = [refs.pop(0) for _ in keys]
    own_a, raw_a, own_b, raw_b, gain, chosen, known, factor = refs
    me = lax.axis_index("mp").astype(jnp.int32)
    for (c, step), resid in zip(keys, own):
        start = lax.rem(me + step, SHARDS) * sum(CHUNKS) + STARTS[c]
        for j in range(0, CHUNKS[c], SLOT):
            at = pl.ds(pl.multiple_of(start + j, SLOT), SLOT)
            branch = jnp.concatenate(
                [
                    own_a[:, at].astype(F32) + raw_a[:, at].astype(F32),
                    own_b[:, at].astype(F32) + raw_b[:, at].astype(F32),
                ],
                0,
            )
            known[:, at] = resid[:, j : j + SLOT].astype(F32) + branch
    factor[...] = gain[...].astype(F32) * chosen[...].astype(F32)


def finish_kernel(known, factor, two_a, two_b, base, adv, occupied, objective_out, total_out):
    width = known.shape[1]
    square = jnp.zeros((SLOT, SLOT), F32)
    product = jnp.zeros((SLOT, SLOT), F32)
    for j in range(0, width, SLOT):
        at = slice(j, j + SLOT)
        two = jnp.concatenate([two_a[:, at].astype(F32), two_b[:, at].astype(F32)], 0)
        rows = (known[:, at] + two).astype(BF16).astype(F32)
        square = square + rows * rows
        product = product + rows * factor[:, at]
    mean = jnp.sum(square, 1, keepdims=True) * (1.0 / width)
    logits = jnp.sum(product, 1, keepdims=True) * lax.rsqrt(mean + norm_eps)
    ratios = jnp.exp(logits - base[...])
    bounded = jnp.clip(ratios, 1.0 - clip_low, 1.0 + clip_high)
    value = jnp.minimum(ratios * adv[...], bounded * adv[...])
    value = jnp.where(occupied[...] > 0.5, value, 0.0)
    diagonal = lax.broadcasted_iota(jnp.int32, (SLOT, SLOT), 1) == lax.broadcasted_iota(
        jnp.int32, (SLOT, SLOT), 0
    )
    line = jnp.sum(jnp.where(diagonal, value, 0.0), 0, keepdims=True)
    objective_out[...] = line
    total = jnp.sum(line, 1, keepdims=True)
    total_out[...] = jnp.broadcast_to(total[None], (SLOT, 1, SLOT))


def body(
    hidden,
    old_logp,
    rewards,
    resp_dest,
    resp_len,
    resp_offset,
    prompt_group,
    attn_gain,
    w_query,
    q_bias,
    w_key,
    k_bias,
    w_value,
    v_bias,
    w_out,
    final_gain,
    chosen_rows,
    log_normalizer,
):
    blocks, later = send_blocks(
        resp_dest,
        resp_len,
        resp_offset,
        prompt_group,
        rewards,
        old_logp.reshape(ROWS, SLOT),
        hidden,
    )
    first_blocks = [blocks[0]] + [None] * (ROWS - 1)
    for chips, other in PARTNERS:
        at = 2 * chips + other
        first_blocks[at] = across(blocks[at], chips, other)
    own_block, near_blocks, other_blocks = later
    from_other = across(other_blocks, 0, 1)
    merged = call(
        merge_kernel,
        [shape(2 * SLOT, CHUNKS[1])] * 3,
        [VMEM] * 2,
        (near_blocks, from_other),
        flops=100000,
        size=1 << 20,
    )
    pairs = [None] * 3
    for chips in (1, 3, 2):
        pairs[chips - 1] = across(merged[chips - 1], chips, 0)

    vector = jnp.concatenate([v.astype(F32) for v in (attn_gain, q_bias, k_bias, v_bias)])[None, :]
    exponents = (np.arange(HEAD) % (HEAD // 2)) * (2.0 / HEAD)
    frequency = jnp.asarray((rope_theta ** (-exponents))[None, :], F32)
    first_blocks[0], vector = lax.optimization_barrier((first_blocks[0], vector))
    upper, lower, positions, notes = pack(0, first_blocks)
    first = gather_halves(upper, lower)
    second = gather_halves(*pack(1, [own_block, from_other, *pairs], notes))
    cosine, sine, *held = settle(positions, frequency, w_query, w_key, w_value, w_out)
    *weights, w_out = [in_vmem(v) for v in held]
    weights = (vector, *weights)
    tables = (cosine, sine)
    carried, own_first = project(0, (0, 1, 3, 2), first, weights)
    carried, own_near = project(1, (0, 1, 3), second, weights, carried)
    far_a, far_b = call(
        functools.partial(far_kernel, 1),
        [shape(SLOT // 2, w_out.shape[1])] * 2,
        [VMEM] * 12,
        (*second[2], *weights, *carried, *tables, positions, w_out),
        flops=10 << 30,
        size=8 << 20,
    )
    carried, far_a, far_b = lax.optimization_barrier((carried, far_a, far_b))
    (queries, keys, values), own_far = project(1, (2,), second, weights, carried, tables)

    attend_to = functools.partial(
        attend,
        queries=queries,
        keys=keys,
        values=values,
        positions=positions,
        w_out=w_out,
    )
    from_left = shift(far_a, "mp", SHARDS, 1)
    from_right = shift(far_b, "mp", SHARDS, -1)
    right_a, right_b, left_a, left_b = attend_to((1, 3))
    raw_b = shift(right_b, "mp", SHARDS, 1)
    raw_a = shift(left_a, "mp", SHARDS, -1)
    notes, left_b = lax.optimization_barrier((notes, left_b))
    stats, mine = call(
        sort_kernel,
        [shape(ROWS, SLOT, dtype=F32), shape(ROWS, 2 * SLOT, dtype=F32)],
        [VMEM],
        (notes,),
        flops=100000,
        size=1 << 17,
    )
    base, adv, occupied, scale = call(
        note_kernel,
        [shape(SLOT, 1, dtype=F32)] * 3 + [shape(1, 1, dtype=F32)],
        [VMEM] * 6,
        (
            stats,
            *[shift(stats, "col", COLS, k) for k in range(1, COLS)],
            mine,
            log_normalizer[None, :],
        ),
        flops=4000000,
        size=1 << 18,
    )
    sum_a, sum_b = call(
        add_kernel,
        [shape(*far_a.shape)] * 2,
        [VMEM] * 4,
        (right_a, from_left, left_b, from_right),
        flops=1000000,
        size=3 << 20,
    )
    two_a = shift(sum_a, "mp", SHARDS, 1)
    two_b = shift(sum_b, "mp", SHARDS, -1)
    own_a, own_b = attend_to((0,))
    final_gain, own_a = lax.optimization_barrier((final_gain, own_a))
    last_gain = final_gain[None, :]

    own = {(0, s): v for s, v in own_first.items()}
    own |= {(1, s): v for s, v in (own_near | own_far).items()}
    names = sorted(own)
    known, factor = call(
        functools.partial(prepare_kernel, names),
        [shape(SLOT, w_out.shape[1], dtype=F32)] * 2,
        [VMEM] * (len(names) + 6),
        (*[own[n] for n in names], own_a, raw_a, own_b, raw_b, last_gain, chosen_rows),
        flops=4000000,
        size=6 << 20,
    )
    objective, totals = call(
        finish_kernel,
        [shape(1, SLOT, dtype=F32), shape(SLOT, 1, SLOT, dtype=F32)],
        [VMEM] * 7,
        (known, factor, two_a, two_b, base, adv, occupied),
        flops=8000000,
        size=6 << 20,
    )
    sums = lax.all_to_all(totals, ROW_COL_MP, 0, 0, tiled=True)
    loss = jnp.sum(sums[:, 0, 0]) * scale[0, 0]
    return objective.reshape(SLOT), loss


def solution(mesh):
    placed = (
        P(ROW_COL, "mp"),
        P(ROW_COL),
        P(ROW_COL),
        P(ROW_COL),
        P(ROW_COL),
        P(ROW_COL),
        P(ROW_COL),
        P(),
        P(None, "mp"),
        P("mp"),
        P(None, "mp"),
        P("mp"),
        P(None, "mp"),
        P("mp"),
        P("mp", None),
        P(),
        P(ROW_COL_MP, None),
        P(ROW_COL_MP),
    )

    return jax.shard_map(
        body, mesh=mesh, in_specs=placed, out_specs=(P(ROW_COL_MP), P()), check_vma=False
    )
```
